768 devices in a mesh: grp: 32 (over x_lo, y, core), tp: 24 (over x_hi, z).
Axes of the slice: x: 4 (x_hi: 2, x_lo: 2; x = x_hi * 2 + x_lo), y: 8, z: 12, core: 2. Of those that a mesh axis runs over, the one named last changes fastest.
Arguments:
- queries: bfloat16 [128, 2, 4096], P('grp'), may hold values from -8 to 8
- cache_keys: bfloat16 [128, 3072, 512], P('grp', 'tp'), may hold values from -8 to 8
- cache_values: bfloat16 [128, 3072, 512], P('grp', 'tp'), may hold values from -6 to 6
- new_keys: bfloat16 [128, 2, 512], P('grp'), may hold values from -6 to 6
- new_values: bfloat16 [128, 2, 512], P('grp'), may hold values from -6 to 6
- lengths: int32 [128], P('grp'), may hold values from 2 to 3072
- residual: bfloat16 [128, 2, 4096], P('grp'), may hold values from -0.1796875 to 0.1796875
- norm_gain: float32 [4096], replicated, may hold values from 0.25 to 1.75
- w_gate: float32 [4096, 14400], P('grp', 'tp'), may hold values from -0.09375 to 0.09375
- w_down: float32 [4096, 14400], P('grp', 'tp'), may hold values from -0.046875 to 0.046875
Outputs:
- mixed: bfloat16 [128, 2, 4096], P('grp')
The draws below stay inside these ranges and needn't reach their ends.
All inputs are finite; a program needn't handle non-finite values.
Results may differ from the reference program's by a relative error of at most 0.028.
Values may be sent and summed in bfloat16 or wider, within the bound.
No kernel may reach another device: no remote copies, remote signals or barrier semaphores. Data moves between devices by JAX's collectives and lax.ppermute only.
A program may use at most 32 MiB of HBM per device.

```python
import jax
import jax.numpy as jnp
from jax import lax

HD = 128
HQ = 32
KVH = 4
STEPS = 2
D = 4096
FF = 14400
ROWS_ALL = 128
CTX = 3072


def draw_queries(key, part):
    values = jax.random.truncated_normal(jax.random.fold_in(key, 11), -6.0, 6.0, (ROWS_ALL, STEPS, HQ * HD), jnp.float32)
    return values.astype(jnp.bfloat16)


def draw_cache_keys(key, part):
    values = jax.random.truncated_normal(jax.random.fold_in(key, 12), -6.0, 6.0, (ROWS_ALL, CTX, KVH * HD), jnp.float32)
    return values.astype(jnp.bfloat16)


def place_ends(drawn, rng, smallest, largest):
    spot = [jax.random.randint(jax.random.fold_in(rng, axis), (), 0, length) for axis, length in enumerate(drawn.shape)]
    main_axis = drawn.shape.index(max(drawn.shape))
    neighbour = spot[:main_axis] + [(spot[main_axis] + 1) % drawn.shape[main_axis]] + spot[main_axis + 1:]
    return drawn.at[tuple(spot)].set(smallest).at[tuple(neighbour)].set(largest)


def block_levels(key, shape, shards, low, largest):
    def one(axis_at, blocks):
        draws = jax.random.uniform(jax.random.fold_in(jax.random.fold_in(key, 6), axis_at), (blocks,), jnp.float32, low / len(shards), largest / len(shards))
        return jnp.repeat(jnp.exp(draws), shape[axis_at] // blocks).reshape((-1,) + (1,) * (len(shape) - axis_at - 1))

    gain = one(*shards[0])
    for cut in shards[1:]:
        gain = gain * one(*cut)
    return gain


def gaussian(key, extent, spread, limit, shards=(), kind=jnp.bfloat16):
    values = jax.random.normal(key, extent, jnp.float32) * spread
    if len(shards) > 0:
        values = block_levels(key, extent, shards, -0.22, 0.18) * values
    return jnp.clip(values, min=-limit, max=limit).astype(kind)


def setup_inputs(seed: int = 0) -> dict:
    streams_of = jax.random.split(jax.random.key(seed), 11)
    queries = draw_queries(jax.random.fold_in(streams_of[10], 71), 0)
    cache_keys = draw_cache_keys(jax.random.fold_in(streams_of[10], 71), 0)
    cache_values = gaussian(streams_of[2], (ROWS_ALL, CTX, KVH * HD), 1.0, 6.0, ((0, 32), (1, 24)))
    new_keys = gaussian(streams_of[3], (ROWS_ALL, STEPS, KVH * HD), 1.0, 6.0, ((0, 32),))
    new_values = gaussian(streams_of[4], (ROWS_ALL, STEPS, KVH * HD), 1.0, 6.0, ((0, 32),))
    lengths = place_ends(jax.random.randint(streams_of[5], (ROWS_ALL,), 2, CTX + 1), jax.random.fold_in(streams_of[5], 1), 2, CTX).astype(jnp.int32)
    residual = gaussian(streams_of[6], (ROWS_ALL, STEPS, D), 0.03, 0.1796875, ((0, 32),))
    norm_gain = jnp.clip(1.0 + 0.15 * jax.random.normal(streams_of[7], (D,), jnp.float32), 0.25, 1.75)
    w_gate = gaussian(streams_of[8], (D, FF), D ** -0.5, 0.09375, ((0, 32), (1, 24)), jnp.float32)
    w_down = gaussian(streams_of[9], (D, FF), FF ** -0.5, 0.046875, ((0, 32), (1, 24)), jnp.float32)
    return {"queries": queries, "cache_keys": cache_keys, "cache_values": cache_values, "new_keys": new_keys, "new_values": new_values, "lengths": lengths, "residual": residual, "norm_gain": norm_gain, "w_gate": w_gate, "w_down": w_down}


masked_score = -1e+30

def reference(queries, cache_keys, cache_values, new_keys, new_values, lengths, residual, norm_gain, w_gate, w_down):
    per_group = HQ // KVH
    inv_root = HD ** (-0.5)
    causal = jnp.arange(STEPS, dtype=jnp.int32)[:, None] >= jnp.arange(STEPS, dtype=jnp.int32)[None, :]
    causal = causal[:, None, None, :]

    def one_row(item):
        query_row, key_rows, value_rows, fresh_keys, fresh_values, length = item
        query_heads = query_row.astype(jnp.float32).reshape(STEPS, KVH, per_group, HD)
        key_heads = key_rows.astype(jnp.float32).reshape(CTX, KVH, HD)
        value_heads = value_rows.astype(jnp.float32).reshape(CTX, KVH, HD)
        fresh_key_heads = fresh_keys.astype(jnp.float32).reshape(STEPS, KVH, HD)
        fresh_value_heads = fresh_values.astype(jnp.float32).reshape(STEPS, KVH, HD)
        visible = jnp.arange(CTX, dtype=jnp.int32) < length
        cached_scores = jnp.einsum('sjgd,cjd->sjgc', query_heads, key_heads) * inv_root
        cached_scores = jnp.where(visible, cached_scores, masked_score)
        fresh_scores = jnp.einsum('sjgd,tjd->sjgt', query_heads, fresh_key_heads) * inv_root
        fresh_scores = jnp.where(causal, fresh_scores, masked_score)
        highest = jnp.maximum(lax.optimization_barrier(jnp.max(cached_scores, axis=-1)), lax.optimization_barrier(jnp.max(fresh_scores, axis=-1)))
        cached_weights = jnp.where(visible, jnp.exp(cached_scores - highest[..., None]), 0.0)
        fresh_weights = jnp.where(causal, jnp.exp(fresh_scores - highest[..., None]), 0.0)
        totals = lax.optimization_barrier(jnp.sum(cached_weights, axis=-1)) + lax.optimization_barrier(jnp.sum(fresh_weights, axis=-1))
        accum = jnp.einsum('sjgc,cjd->sjgd', cached_weights.astype(jnp.bfloat16).astype(jnp.float32), value_heads)
        accum = accum + jnp.einsum('sjgt,tjd->sjgd', fresh_weights.astype(jnp.bfloat16).astype(jnp.float32), fresh_value_heads)
        return (accum / totals[..., None]).reshape(STEPS, HQ * HD)
    context = lax.map(one_row, (queries, cache_keys, cache_values, new_keys, new_values, lengths))
    summed = residual.astype(jnp.float32) + context
    mean_square = lax.optimization_barrier(jnp.mean(summed * summed, axis=-1, keepdims=True))
    normed = (summed * lax.rsqrt(mean_square + 1e-05) * norm_gain.astype(jnp.float32)).astype(jnp.bfloat16)
    flat = normed.reshape(ROWS_ALL * STEPS, D)
    gate = jnp.dot(flat, w_gate.astype(jnp.bfloat16), preferred_element_type=jnp.float32)
    hidden = jax.nn.silu(gate).astype(jnp.bfloat16)
    mlp = lax.dot_general(hidden, w_down.astype(jnp.bfloat16), (((1,), (1,)), ((), ())), preferred_element_type=jnp.float32)
    return (summed + mlp.reshape(ROWS_ALL, STEPS, D)).astype(jnp.bfloat16)
```

```python
import jax
import jax.numpy as jnp
from jax import lax
from jax.sharding import Mesh
from jax.sharding import PartitionSpec as P

HD = 128
KVH = 4
HQ = 32
GRP = ("xl", "y", "c")
TP = ("xh", "z")
WIDE = ("xl", "y", "c", "xh")
CHUNK = 20
NEAR = 24
masked_score = -1e30


def exchange(parts, axis):
    return lax.all_to_all(parts, axis, split_axis=0, concat_axis=0, tiled=True)


def copies(part, axis):
    return exchange(jnp.broadcast_to(part, (lax.axis_size(axis), *part.shape)), axis)


def two_words(value):
    high = value.astype(jnp.bfloat16)
    return high, (value - high.astype(jnp.float32)).astype(jnp.bfloat16)


def pad_to(array, axis, size):
    widths = [(0, 0)] * array.ndim
    widths[axis] = (0, size - array.shape[axis])
    return jnp.pad(array, widths)


def resharded(w_gate, w_down, groups, slices, per_slice):
    stacked = jnp.stack([w_gate.T, w_down.T]).astype(jnp.bfloat16)
    stacked = pad_to(stacked, 1, groups * CHUNK)
    parts = jnp.moveaxis(stacked.reshape(2, groups, CHUNK, HD), 0, 1)
    heads = exchange(parts, GRP)
    heads = pad_to(heads, 0, slices * per_slice)
    arrived = exchange(heads.reshape(slices, per_slice, 2, CHUNK, HD), "z")
    both = jnp.transpose(arrived, (2, 0, 3, 1, 4)).reshape(2, slices * CHUNK, per_slice * HD)
    return both[0], both[1]


def shards(
    queries,
    cache_keys,
    cache_values,
    new_keys,
    new_values,
    lengths,
    residual,
    norm_gain,
    w_gate,
    w_down,
):
    rows, steps, features = queries.shape
    positions = cache_keys.shape[1]
    groups, slices, halves = lax.axis_size(GRP), lax.axis_size("z"), lax.axis_size("xh")
    per_slice = -(-HQ // slices)
    slots = slices * per_slice
    wide = per_slice * HD
    tokens = rows * steps
    share = tokens // halves
    total_tokens = groups * tokens
    gate_weights, down_weights = resharded(w_gate, w_down, groups, slices, per_slice)

    per_group = HQ // KVH
    inv_root = HD ** (-0.5)
    here = lax.axis_index(TP)
    query_heads = queries.reshape(rows, steps, KVH, per_group, HD)
    key_heads = cache_keys.reshape(rows, positions, KVH, HD)
    value_heads = cache_values.reshape(rows, positions, KVH, HD)
    scores = jnp.einsum("rsjgd,rcjd->rsjgc", query_heads, key_heads, preferred_element_type=jnp.float32) * inv_root
    places = here * positions + lax.broadcasted_iota(jnp.int32, (rows, positions), 1)
    visible = (places < lengths[:, None])[:, None, None, None, :]
    scores = jnp.where(visible, scores, masked_score)
    fresh = jnp.einsum(
        "rsjgd,rtjd->rsjgt", query_heads, new_keys.reshape(rows, steps, KVH, HD), preferred_element_type=jnp.float32
    ) * inv_root
    causal = lax.broadcasted_iota(jnp.int32, (steps, steps), 0) >= lax.broadcasted_iota(jnp.int32, (steps, steps), 1)
    causal = (causal & (here == 0))[None, :, None, None, :]
    fresh = jnp.where(causal, fresh, masked_score)
    highest = jnp.maximum(jnp.max(scores, axis=-1), jnp.max(fresh, axis=-1))
    shift = highest.astype(jnp.bfloat16)
    shift_wide = lax.reduce_precision(highest, 8, 7)[..., None]
    weights = jnp.where(visible, jnp.exp(scores - shift_wide), 0.0)
    fresh_weights = jnp.where(causal, jnp.exp(fresh - shift_wide), 0.0)
    totals = jnp.sum(weights, axis=-1) + jnp.sum(fresh_weights, axis=-1)
    accum = jnp.einsum(
        "rsjgc,rcjd->rsjgd", weights.astype(jnp.bfloat16), value_heads, preferred_element_type=jnp.float32
    ) + jnp.einsum(
        "rsjgt,rtjd->rsjgd",
        fresh_weights.astype(jnp.bfloat16),
        new_values.reshape(rows, steps, KVH, HD),
        preferred_element_type=jnp.float32,
    )

    def by_target(array):
        array = pad_to(array.reshape(halves, share, HQ, -1), 2, slots)
        array = array.reshape(halves, share, slices, per_slice, -1)
        return jnp.transpose(array, (0, 2, 1, 3, 4)).reshape(halves * slices, share * per_slice, -1)

    high, low = two_words(totals)
    stats = by_target(jnp.stack([shift, high, low], axis=-1))
    stats = pad_to(pad_to(jnp.swapaxes(stats, 1, 2), 2, HD), 1, 4)
    sent = jnp.concatenate([by_target(accum.astype(jnp.bfloat16)), stats], axis=1)
    pieces = exchange(sent, TP)

    lines = share * per_slice
    stats = pieces[:, lines:, :lines].astype(jnp.float32)
    joint = jnp.max(stats[:, 0], axis=0)
    factor = jnp.exp(stats[:, 0] - joint)
    total = jnp.sum(factor * (stats[:, 1] + stats[:, 2]), axis=0)
    total = jnp.where(total > 0, total, 1.0)
    context = jnp.sum(factor[..., None] * pieces[:, :lines].astype(jnp.float32), axis=0) / total[:, None]

    half, at = lax.axis_index("xh"), lax.axis_index("z")
    mine = pad_to(residual.reshape(tokens, features), 1, slots * HD)
    mine = lax.dynamic_slice(mine, (half * share, at * wide), (share, wide))
    gain = lax.dynamic_slice(jnp.pad(norm_gain, (0, slots * HD - features), constant_values=1.0), (at * wide,), (wide,))
    summed = mine.astype(jnp.float32) + context.reshape(share, wide)
    gained = copies((summed * gain).astype(jnp.bfloat16), WIDE).reshape(total_tokens, wide)

    unscaled = gained.astype(jnp.float32) / gain
    squares = jnp.stack(two_words(jnp.sum(unscaled * unscaled, axis=-1)), axis=-1)
    gate = lax.dot_general(gained, gate_weights, (((1,), (1,)), ((), ())), preferred_element_type=jnp.float32)
    sent = jnp.concatenate([gate.astype(jnp.bfloat16), squares], axis=-1)
    sent = pad_to(sent, 0, slices * NEAR).reshape(slices, NEAR, -1)
    arrived = exchange(sent, "z").astype(jnp.float32).sum(axis=0)
    units = gate_weights.shape[0]
    mean_square = (arrived[:, units] + arrived[:, units + 1]) / features
    gate = arrived[:, :units] * lax.rsqrt(mean_square + 1e-05)[:, None]
    hidden = jax.nn.silu(gate).astype(jnp.bfloat16)
    hidden = copies(hidden, "z").reshape(slices * NEAR, units)[:total_tokens]
    terms = jnp.dot(hidden, down_weights, preferred_element_type=jnp.float32).astype(jnp.bfloat16)
    mlp = exchange(terms.reshape(groups * halves, share, wide), WIDE).astype(jnp.float32).sum(axis=0)
    mixed = copies((summed + mlp).astype(jnp.bfloat16), TP)
    mixed = jnp.swapaxes(mixed.reshape(halves, slices, share, wide), 1, 2)
    return mixed.reshape(rows, steps, slots * HD)[..., :features]


def solution(mesh):
    fine = Mesh(mesh.devices.reshape(2, 8, 2, 2, 12), ("xl", "y", "c", "xh", "z"))
    return jax.shard_map(
        shards,
        mesh=fine,
        in_specs=(
            P(GRP, None, None),
            P(GRP, TP, None),
            P(GRP, TP, None),
            P(GRP, None, None),
            P(GRP, None, None),
            P(GRP),
            P(GRP, None, None),
            P(),
            P(GRP, TP),
            P(GRP, TP),
        ),
        out_specs=P(GRP, None, None),
        check_vma=False,
    )
```

```python
import jax
import jax.numpy as jnp
from jax import lax
from jax.sharding import Mesh
from jax.sharding import PartitionSpec as P

HD = 128
KVH = 4
HQ = 32
GRP = ("xl", "ya", "yb", "c")
TP = ("xh", "z2", "z1")
WIDE = ("xl", "ya", "yb", "c", "xh")
DEEP = ("xl", "c", "z1")
HALF = 304
masked_score = -1e30


def exchange(parts, axis):
    return lax.all_to_all(parts, axis, split_axis=0, concat_axis=0, tiled=True)


def copies(part, axis):
    return exchange(jnp.broadcast_to(part, (lax.axis_size(axis), *part.shape)), axis)


def two_words(value):
    high = value.astype(jnp.bfloat16)
    return high, (value - high.astype(jnp.float32)).astype(jnp.bfloat16)


def pad_to(array, axis, size):
    widths = [(0, 0)] * array.ndim
    widths[axis] = (0, size - array.shape[axis])
    return jnp.pad(array, widths)


def traded(halves, other):
    near = lax.axis_size("ya")
    moves = []
    for row in range(near):
        for pair in range(2):
            for deep in range(near):
                target = (deep * 2 + (pair ^ other)) * near + row
                moves.append(((row * 2 + pair) * near + deep, target))
    at = lax.axis_index("yb") ^ other
    return lax.ppermute(lax.dynamic_index_in_dim(halves, at, 1, False), ("ya", "yb", "z1"), moves)


def shards(
    queries,
    cache_keys,
    cache_values,
    new_keys,
    new_values,
    lengths,
    residual,
    norm_gain,
    w_gate,
    w_down,
):
    rows, steps, features = queries.shape
    positions = cache_keys.shape[1]
    groups, halves = lax.axis_size(GRP), lax.axis_size("xh")
    tokens = rows * steps
    share = tokens // halves
    total_tokens = groups * tokens
    near = lax.axis_size("z1")
    far = lax.axis_size("z2")

    stacked = jnp.stack([w_gate.T, w_down.T]).astype(jnp.bfloat16)
    stacked = pad_to(stacked, 1, 2 * HALF).reshape(2, 2, HALF, HD)
    own, other = traded(stacked, 0), traded(stacked, 1)

    per_group = HQ // KVH
    inv_root = HD ** (-0.5)
    here = lax.axis_index(TP)
    query_heads = queries.reshape(rows, steps, KVH, per_group, HD)
    key_heads = cache_keys.reshape(rows, positions, KVH, HD)
    value_heads = cache_values.reshape(rows, positions, KVH, HD)
    scores = jnp.einsum("rsjgd,rcjd->rsjgc", query_heads, key_heads, preferred_element_type=jnp.float32) * inv_root
    places = here * positions + lax.broadcasted_iota(jnp.int32, (rows, positions), 1)
    visible = (places < lengths[:, None])[:, None, None, None, :]
    scores = jnp.where(visible, scores, masked_score)
    fresh = jnp.einsum(
        "rsjgd,rtjd->rsjgt", query_heads, new_keys.reshape(rows, steps, KVH, HD), preferred_element_type=jnp.float32
    ) * inv_root
    causal = lax.broadcasted_iota(jnp.int32, (steps, steps), 0) >= lax.broadcasted_iota(jnp.int32, (steps, steps), 1)
    causal = (causal & (here == 0))[None, :, None, None, :]
    fresh = jnp.where(causal, fresh, masked_score)
    highest = jnp.maximum(jnp.max(scores, axis=-1), jnp.max(fresh, axis=-1))
    shift = highest.astype(jnp.bfloat16)
    shift_wide = lax.reduce_precision(highest, 8, 7)[..., None]
    weights = jnp.where(visible, jnp.exp(scores - shift_wide), 0.0)
    fresh_weights = jnp.where(causal, jnp.exp(fresh - shift_wide), 0.0)
    totals = jnp.sum(weights, axis=-1) + jnp.sum(fresh_weights, axis=-1)
    accum = jnp.einsum(
        "rsjgc,rcjd->rsjgd", weights.astype(jnp.bfloat16), value_heads, preferred_element_type=jnp.float32
    ) + jnp.einsum(
        "rsjgt,rtjd->rsjgd",
        fresh_weights.astype(jnp.bfloat16),
        new_values.reshape(rows, steps, KVH, HD),
        preferred_element_type=jnp.float32,
    )

    lines = share * 2 * 4

    def by_target(array):
        array = array.reshape(halves, share, 2, near, 4, -1)
        return jnp.transpose(array, (0, 3, 1, 2, 4, 5)).reshape(halves, near, lines, -1)

    high, low = two_words(totals)
    stats = by_target(jnp.stack([shift, high, low], axis=-1))
    stats = pad_to(jnp.swapaxes(stats, 2, 3).reshape(halves, near, 1, 3 * lines), 3, HD)
    sent = jnp.concatenate([by_target(accum.astype(jnp.bfloat16)), stats], axis=2)
    sent = jnp.broadcast_to(sent[:, None], (halves, far, near, lines + 1, HD))
    pieces = exchange(sent.reshape(halves * far * near, lines + 1, HD), TP)

    stats = pieces[:, lines, : 3 * lines].astype(jnp.float32).reshape(-1, 3, lines)
    joint = jnp.max(stats[:, 0], axis=0)
    factor = jnp.exp(stats[:, 0] - joint)
    total = jnp.sum(factor * (stats[:, 1] + stats[:, 2]), axis=0)
    context = jnp.sum(factor[..., None] * pieces[:, :lines].astype(jnp.float32), axis=0) / total[:, None]

    half, deep = lax.axis_index("xh"), lax.axis_index("z1")
    mine = residual.reshape(halves, share, 2, near, 4, HD)
    mine = lax.dynamic_index_in_dim(lax.dynamic_index_in_dim(mine, half, 0, False), deep, 2, False)
    gain = lax.dynamic_index_in_dim(norm_gain.reshape(2, near, 4, HD), deep, 1, False)
    summed = mine.astype(jnp.float32) + context.reshape(share, 2, 4, HD)
    gained = (summed * gain).astype(jnp.bfloat16).reshape(share, 2, 2, 2, HD)
    gained = jnp.transpose(gained, (1, 3, 0, 2, 4))
    ordered = jnp.stack([gained, gained[:, :, :, ::-1]], axis=1)
    ordered = jnp.broadcast_to(ordered[:, None, :, :, None], (2, near, 2, 2, halves, share, 2, HD))
    arrived = exchange(ordered.reshape(groups * halves, share, 2 * HD), WIDE).reshape(total_tokens, 2 * HD)

    pair = lax.axis_index("yb")
    gain = gain.reshape(2, 2, 2, HD)[lax.axis_index("xl"), :, lax.axis_index("c")]
    gain = jnp.where(pair == 0, gain, gain[::-1]).reshape(2 * HD)
    unscaled = arrived.astype(jnp.float32) / gain
    squares = jnp.stack(two_words(jnp.sum(unscaled * unscaled, axis=-1)), axis=-1)
    turned = (((1,), (1,)), ((), ()))
    gate = lax.dot_general(arrived[:, :HD], own[0], turned, preferred_element_type=jnp.float32)
    gate = gate + lax.dot_general(arrived[:, HD:], other[0], turned, preferred_element_type=jnp.float32)
    sent = jnp.concatenate([gate.astype(jnp.bfloat16), squares], axis=-1)
    depth = lax.axis_size(DEEP)
    sums = exchange(sent.reshape(depth, total_tokens // depth, -1), DEEP).astype(jnp.float32).sum(axis=0)
    mean_square = (sums[:, HALF] + sums[:, HALF + 1]) / features
    gate = sums[:, :HALF] * lax.rsqrt(mean_square + 1e-05)[:, None]
    hidden = copies(jax.nn.silu(gate).astype(jnp.bfloat16), DEEP).reshape(total_tokens, HALF)
    terms = jnp.concatenate(
        [jnp.dot(hidden, w[1], preferred_element_type=jnp.float32).astype(jnp.bfloat16) for w in (own, other)], axis=-1
    )
    partial = exchange(terms.reshape(groups * halves, share, 2 * HD), WIDE)
    partial = partial.reshape(2, near, 2, 2, halves, share, 2, HD).astype(jnp.float32).sum(axis=(1, 4))
    mlp = partial[:, 0] + partial[:, 1, :, :, ::-1]
    mlp = jnp.transpose(mlp, (2, 0, 3, 1, 4)).reshape(share, 2, 4, HD)
    mixed = mlp + jnp.where(lax.axis_index("z2") == 0, summed, 0.0)
    mixed = copies(mixed.astype(jnp.bfloat16).reshape(share, 8 * HD), TP)
    mixed = mixed.reshape(halves, far, near, share, 2, 4, HD).astype(jnp.float32).sum(axis=1)
    mixed = jnp.transpose(mixed, (0, 2, 3, 1, 4, 5))
    return mixed.astype(jnp.bfloat16).reshape(rows, steps, features)


def solution(mesh):
    fine = Mesh(mesh.devices.reshape(2, 4, 2, 2, 2, 3, 4), ("xl", "ya", "yb", "c", "xh", "z2", "z1"))
    return jax.shard_map(
        shards,
        mesh=fine,
        in_specs=(
            P(GRP, None, None),
            P(GRP, TP, None),
            P(GRP, TP, None),
            P(GRP, None, None),
            P(GRP, None, None),
            P(GRP),
            P(GRP, None, None),
            P(),
            P(GRP, TP),
            P(GRP, TP),
        ),
        out_specs=P(GRP, None, None),
        check_vma=False,
    )
```

```python
import jax
import jax.numpy as jnp
from jax import lax
from jax.experimental import pallas as pl
from jax.experimental.pallas import tpu as pltpu
from jax.sharding import Mesh
from jax.sharding import PartitionSpec as P


HD = 128
KVH = 4
HQ = 32
EACH = HQ // KVH
PER = 3
GRP = ("xl", "y", "c")
TP = ("xh", "z")
WIDE = ("xl", "y", "c", "xh")
HALF = 304
NEAR = 24
masked_score = -1e30
ANY = pl.BlockSpec(memory_space=pl.ANY)


def exchange(parts, axis):
    return lax.all_to_all(parts, axis, split_axis=0, concat_axis=0, tiled=True)


def copies(part, axis):
    return exchange(jnp.broadcast_to(part, (lax.axis_size(axis), *part.shape)), axis)


def two_words(value):
    high = value.astype(jnp.bfloat16)
    return high, (value - high.astype(jnp.float32)).astype(jnp.bfloat16)


def pad_to(array, axis, size, fill=0):
    widths = [(0, 0)] * array.ndim
    widths[axis] = (0, size - array.shape[axis])
    return jnp.pad(array, widths, constant_values=fill)


def by_slot(array, axis, fill=0):
    shape = array.shape
    array = array.reshape(*shape[:axis], KVH, EACH, *shape[axis + 1 :])
    array = pad_to(array, axis + 1, 3 * PER, fill)
    return array.reshape(*shape[:axis], 3 * KVH, PER, *shape[axis + 1 :])


def moved(halves, turn):
    slices = lax.axis_size("z")
    moves = []
    for head in range(HQ):
        half = (turn - head % EACH % PER) % PER
        if half > 1:
            continue
        deep = head // EACH * 3 + head % EACH // PER
        for at in range(slices):
            moves.append((head * slices + at, (at * 2 + half) * slices + deep))
    slot = lax.rem(lax.rem(lax.axis_index(GRP), EACH), PER)
    half = jnp.minimum(lax.rem(turn - slot + PER, PER), 1)
    sent = lax.dynamic_index_in_dim(halves, half, 1, False)
    return lax.ppermute(sent, (*GRP, "z"), moves)


def attend(lengths_ref, here_ref, q_hbm, k_hbm, v_hbm, nk_hbm, nv_hbm, out_ref, q, k, v, nk, nv, small, large):
    rows, positions = k.shape[0], k.shape[1]
    half_rows = rows // 2
    first = [pltpu.make_async_copy(s, d, small.at[i]) for i, (s, d) in enumerate(((q_hbm, q), (nk_hbm, nk), (nv_hbm, nv)))]
    keys = [pltpu.make_async_copy(k_hbm.at[r], k.at[r], large.at[0, r]) for r in range(rows)]
    values = [pltpu.make_async_copy(v_hbm.at[r], v.at[r], large.at[1, r]) for r in range(rows)]
    for copy in first:
        copy.start()
    for r in range(rows):
        keys[r].start()
        values[r].start()
    here = here_ref[0]
    lines = half_rows * 2 * EACH

    def of_line(line):
        each = lax.rem(line, EACH)
        return lax.div(each, PER), lax.div(line, EACH) * PER + lax.rem(each, PER)

    out_line = lax.broadcasted_iota(jnp.int32, (3 * 16, 4 * lines), 0)
    source = lax.broadcasted_iota(jnp.int32, (3 * 16, 4 * lines), 1)
    block, zone_of = lax.div(source, lines), None
    zone_of, slot_of = of_line(lax.rem(source, lines))
    place = lax.rem(out_line, 16)
    wanted = jnp.where(block == 0, slot_of, half_rows * 2 * PER + block - 1)
    select = jnp.where((lax.div(out_line, 16) == zone_of) & (place == wanted), 1.0, 0.0).astype(jnp.bfloat16)
    line = lax.broadcasted_iota(jnp.int32, (lines, HD), 0)
    lane = lax.broadcasted_iota(jnp.int32, (lines, HD), 1)
    spread = of_line(line)[1] == lane
    step = lax.div(lax.broadcasted_iota(jnp.int32, (2 * EACH, 1), 0), EACH)
    fresh_ok = [(here == 0) & (step >= t) for t in range(2)]
    position = lax.broadcasted_iota(jnp.int32, (2 * EACH, positions), 1) + here * positions
    for copy in first:
        copy.wait()
    turned = (((1,), (1,)), ((), ()))
    for half in range(2):
        for r in range(half * half_rows, (half + 1) * half_rows):
            keys[r].wait()
            values[r].wait()
        for j in range(KVH):
            at = pl.ds(j * HD, HD)
            parts = []
            for r in range(half * half_rows, (half + 1) * half_rows):
                query = q[r, j]
                visible = position < lengths_ref[r]
                scores = lax.dot_general(query, k[r, :, at], turned, preferred_element_type=jnp.float32) * HD**-0.5
                scores = jnp.where(visible, scores, masked_score)
                wide = query.astype(jnp.float32)
                fresh = [
                    jnp.where(
                        fresh_ok[t],
                        jnp.sum(wide * nk[r, t : t + 1, at].astype(jnp.float32), axis=1, keepdims=True) * HD**-0.5,
                        masked_score,
                    )
                    for t in range(2)
                ]
                top = jnp.maximum(jnp.max(scores, axis=1, keepdims=True), jnp.maximum(*fresh))
                shift = top.astype(jnp.bfloat16).astype(jnp.float32)
                weights = jnp.where(visible, jnp.exp(scores - shift), 0.0)
                added = [jnp.where(fresh_ok[t], jnp.exp(fresh[t] - shift), 0.0) for t in range(2)]
                total = jnp.sum(weights, axis=1, keepdims=True) + added[0] + added[1]
                accum = jnp.dot(weights.astype(jnp.bfloat16), v[r, :, at], preferred_element_type=jnp.float32)
                for t in range(2):
                    accum += added[t].astype(jnp.bfloat16).astype(jnp.float32) * nv[r, t : t + 1, at].astype(jnp.float32)
                parts.append((accum, shift, total))
            accum, shift, total = (jnp.concatenate(list(p), axis=0) for p in zip(*parts))
            high = total.astype(jnp.bfloat16).astype(jnp.float32)
            stacked = jnp.concatenate(
                [accum] + [jnp.where(spread, stat, 0.0) for stat in (shift, high, total - high)], axis=0
            ).astype(jnp.bfloat16)
            chosen = jnp.dot(select, stacked, preferred_element_type=jnp.float32).astype(jnp.bfloat16)
            out_ref[pl.ds((half * KVH + j) * 3, 3)] = chosen.reshape(3, 16, HD)


def attention(queries, cache_keys, cache_values, new_keys, new_values, lengths, here):
    rows, steps, _ = queries.shape
    queries = jnp.swapaxes(queries.reshape(rows, steps, KVH, EACH, HD), 1, 2).reshape(rows, KVH, steps * EACH, HD)
    kinds = (queries, cache_keys, cache_values, new_keys, new_values)
    smem = pl.BlockSpec(memory_space=pltpu.SMEM)
    return pl.pallas_call(
        attend,
        out_shape=jax.ShapeDtypeStruct((2 * 3 * KVH, 16, HD), jnp.bfloat16),
        in_specs=[smem, smem] + [ANY] * 5,
        out_specs=pl.BlockSpec(memory_space=pltpu.VMEM),
        scratch_shapes=[pltpu.VMEM(a.shape, a.dtype) for a in kinds]
        + [pltpu.SemaphoreType.DMA((3,)), pltpu.SemaphoreType.DMA((2, rows))],
        cost_estimate=pl.CostEstimate(flops=10**8, bytes_accessed=1 << 20, transcendentals=1 << 15),
        name="attend",
    )(lengths, here, *kinds)


def layer(
    queries,
    cache_keys,
    cache_values,
    new_keys,
    new_values,
    lengths,
    residual,
    norm_gain,
    w_gate,
    w_down,
):
    rows, steps, features = queries.shape
    groups, halves, slices = lax.axis_size(GRP), lax.axis_size("xh"), lax.axis_size("z")
    tokens = rows * steps
    share = tokens // halves
    total_tokens = groups * tokens
    wide = PER * HD

    stacked = jnp.stack([w_gate.T, w_down.T]).astype(jnp.bfloat16)
    stacked = pad_to(stacked, 1, 2 * HALF).reshape(2, 2, HALF, HD)
    weights = [moved(stacked, turn) for turn in range(PER)]

    here = lax.axis_index(TP).reshape(1)
    sent = attention(queries, cache_keys, cache_values, new_keys, new_values, lengths, here)
    pieces = exchange(sent, TP)

    lines = share * PER
    stats = pieces[:, lines : lines + 3, :lines].astype(jnp.float32)
    joint = jnp.max(stats[:, 0], axis=0)
    factor = jnp.exp(stats[:, 0] - joint)
    total = jnp.sum(factor * (stats[:, 1] + stats[:, 2]), axis=0)
    total = jnp.where(total > 0, total, 1.0)
    context = jnp.sum(factor[..., None] * pieces[:, :lines].astype(jnp.float32), axis=0) / total[:, None]

    half, deep = lax.axis_index("xh"), lax.axis_index("z")
    mine = by_slot(residual.reshape(halves, share, HQ, HD), 2)
    mine = lax.dynamic_index_in_dim(lax.dynamic_index_in_dim(mine, half, 0, False), deep, 1, False)
    gain = lax.dynamic_index_in_dim(by_slot(norm_gain.reshape(HQ, HD), 0, 1.0), deep, 0, False)
    summed = mine.astype(jnp.float32) + context.reshape(share, PER, HD)
    gained = (summed * gain).astype(jnp.bfloat16)
    ordered = jnp.stack([gained, jnp.roll(gained, 1, axis=1)])
    ordered = jnp.broadcast_to(ordered[None, :, None], (groups // 2, 2, halves, share, PER, HD))
    gain = jnp.where(lax.axis_index("c") == 0, gain, jnp.roll(gain, 1, axis=0)).reshape(wide)
    ordered, gain, summed = lax.optimization_barrier((ordered.reshape(groups * halves, share, wide), gain, summed))
    arrived = exchange(ordered, WIDE)
    arrived = arrived.reshape(total_tokens, wide)

    unscaled = arrived.astype(jnp.float32) / gain
    squares = jnp.stack(two_words(jnp.sum(unscaled * unscaled, axis=-1)), axis=-1)
    turned = (((1,), (1,)), ((), ()))
    gate = sum(
        lax.dot_general(arrived[:, k * HD : (k + 1) * HD], w[0], turned, preferred_element_type=jnp.float32)
        for k, w in enumerate(weights)
    )
    sent = jnp.concatenate([gate.astype(jnp.bfloat16), squares], axis=-1)
    sent = pad_to(sent, 0, slices * NEAR).reshape(slices, NEAR, -1)
    sums = exchange(sent, "z").astype(jnp.float32).sum(axis=0)
    mean_square = (sums[:, HALF] + sums[:, HALF + 1]) / features
    gate = sums[:, :HALF] * lax.rsqrt(mean_square + 1e-05)[:, None]
    hidden = copies(jax.nn.silu(gate).astype(jnp.bfloat16), "z").reshape(slices * NEAR, HALF)[:total_tokens]
    terms = jnp.concatenate(
        [jnp.dot(hidden, w[1], preferred_element_type=jnp.float32).astype(jnp.bfloat16) for w in weights], axis=-1
    )
    terms, summed = lax.optimization_barrier((terms.reshape(groups * halves, share, wide), summed))
    partial = exchange(terms, WIDE).reshape(groups // 2, 2, halves, share, PER, HD)
    partial = partial.astype(jnp.float32).sum(axis=(0, 2))
    mixed = summed + partial[0] + jnp.roll(partial[1], -1, axis=1)
    mixed = copies(mixed.astype(jnp.bfloat16).reshape(share, wide), TP)
    mixed = jnp.swapaxes(mixed.reshape(halves, KVH, 3, share, PER, HD), 2, 3)
    mixed = jnp.swapaxes(mixed, 1, 2).reshape(tokens, KVH, 3 * PER, HD)[:, :, :EACH]
    return mixed.reshape(rows, steps, features)


def solution(mesh):
    fine = Mesh(mesh.devices.reshape(2, 8, 2, 2, 12), ("xl", "y", "c", "xh", "z"))
    return jax.shard_map(
        layer,
        mesh=fine,
        in_specs=(
            P(GRP, None, None),
            P(GRP, TP, None),
            P(GRP, TP, None),
            P(GRP, None, None),
            P(GRP, None, None),
            P(GRP),
            P(GRP, None, None),
            P(),
            P(GRP, TP),
            P(GRP, TP),
        ),
        out_specs=P(GRP, None, None),
        check_vma=False,
    )
```

```python
import jax
import jax.numpy as jnp
from jax import lax
from jax.experimental import pallas as pl
from jax.experimental.pallas import tpu as pltpu
from jax.sharding import Mesh
from jax.sharding import PartitionSpec as P


HD = 128
KVH = 4
HQ = 32
EACH = HQ // KVH
NEAR = 4
FAR = 3
LINES = 32
GRP = ("xl", "ya", "yb", "c")
TP = ("xh", "z2", "z1")
WIDE = ("xl", "ya", "yb", "c", "xh")
DEEP = ("xl", "c", "z1")
HALF = 304
masked_score = -1e30


def exchange(parts, axis):
    return lax.all_to_all(parts, axis, split_axis=0, concat_axis=0, tiled=True)


def copies(part, axis):
    return exchange(jnp.broadcast_to(part, (lax.axis_size(axis), *part.shape)), axis)


def two_words(value):
    high = value.astype(jnp.bfloat16)
    return high, (value - high.astype(jnp.float32)).astype(jnp.bfloat16)


def pad_to(array, axis, size):
    widths = [(0, 0)] * array.ndim
    widths[axis] = (0, size - array.shape[axis])
    return jnp.pad(array, widths)


def traded(halves, other):
    near = lax.axis_size("ya")
    moves = []
    for row in range(near):
        for pair in range(2):
            for deep in range(near):
                target = (deep * 2 + (pair ^ other)) * near + row
                moves.append(((row * 2 + pair) * near + deep, target))
    at = lax.axis_index("yb") ^ other
    sent = lax.dynamic_index_in_dim(halves, at, 1, False)
    return lax.ppermute(sent, ("ya", "yb", "z1"), moves)


def attend(lengths_ref, here_ref, q_hbm, k_hbm, v_hbm, nk_hbm, nv_hbm, out_ref, q, k, v, nk, nv, small, large):
    rows, positions = k.shape[0], k.shape[1]
    pairs = ((q_hbm, q), (nk_hbm, nk), (nv_hbm, nv))
    first = [pltpu.make_async_copy(s, d, small.at[i]) for i, (s, d) in enumerate(pairs)]
    keys = [pltpu.make_async_copy(k_hbm.at[r], k.at[r], large.at[0, r]) for r in range(rows)]
    values = [pltpu.make_async_copy(v_hbm.at[r], v.at[r], large.at[1, r]) for r in range(rows)]
    for copy in first + keys + values:
        copy.start()
    here = here_ref[0]
    block = 2 * EACH
    lines = rows * KVH * block
    each_row = KVH * block
    step = lax.rem(lax.broadcasted_iota(jnp.int32, (lines, 1), 0), 2)
    fresh_ok = [(here == 0) & (step >= t) for t in range(2)]
    lane = lax.broadcasted_iota(jnp.int32, (each_row, positions), 1) + here * positions
    visible = jnp.concatenate([lane < lengths_ref[r] for r in range(rows)], axis=0)

    def all_lines(part):
        return jnp.concatenate([part(r, j) for r in range(rows) for j in range(KVH)], axis=0)

    def head_of(ref, r, j):
        return ref[r, :, j * HD : (j + 1) * HD]

    for copy in first:
        copy.wait()
    queries = []
    for r in range(rows):
        row = q[r].astype(jnp.float32)
        queries += [row[:, h * HD : (h + 1) * HD] for h in range(HQ)]
    queries = jnp.concatenate(queries, axis=0)
    narrow = queries.astype(jnp.bfloat16)

    def fresh_of(ref, t):
        return all_lines(
            lambda r, j: jnp.broadcast_to(ref[r, t : t + 1, j * HD : (j + 1) * HD].astype(jnp.float32), (block, HD))
        )

    fresh = [
        jnp.where(fresh_ok[t], jnp.sum(queries * fresh_of(nk, t), axis=1, keepdims=True) * HD**-0.5, masked_score)
        for t in range(2)
    ]
    for copy in keys:
        copy.wait()

    def lines_of(array, r, j):
        at = (r * KVH + j) * block
        return array[at : at + block]

    turned = (((1,), (1,)), ((), ()))
    scores = all_lines(
        lambda r, j: lax.dot_general(
            lines_of(narrow, r, j), head_of(k, r, j), turned, preferred_element_type=jnp.float32
        )
    )
    scores = jnp.where(visible, scores * HD**-0.5, masked_score)
    top = jnp.maximum(jnp.max(scores, axis=1, keepdims=True), jnp.maximum(*fresh))
    shift = top.astype(jnp.bfloat16).astype(jnp.float32)
    weights = jnp.where(visible, jnp.exp(scores - shift), 0.0)
    added = [jnp.where(fresh_ok[t], jnp.exp(fresh[t] - shift), 0.0) for t in range(2)]
    total = jnp.sum(weights, axis=1, keepdims=True) + added[0] + added[1]
    weights = weights.astype(jnp.bfloat16)
    for copy in values:
        copy.wait()
    accum = all_lines(
        lambda r, j: jnp.dot(lines_of(weights, r, j), head_of(v, r, j), preferred_element_type=jnp.float32)
    )
    for t in range(2):
        accum += added[t].astype(jnp.bfloat16).astype(jnp.float32) * fresh_of(nv, t)
    high = total.astype(jnp.bfloat16).astype(jnp.float32)
    line = lax.broadcasted_iota(jnp.int32, (LINES, HD), 0)
    offset = lax.broadcasted_iota(jnp.int32, (LINES, HD), 1) - line
    for half in range(2):
        for near in range(NEAR):

            def lines_to(array):
                parts = []
                for r in range(half * rows // 2, (half + 1) * rows // 2):
                    for side in range(2):
                        at = (r * KVH + side * 2 + near // 2) * block + near % 2 * 8
                        parts.append(array[at : at + 8])
                return jnp.concatenate(parts, axis=0)

            lead = lines_to(high)
            stats = jnp.where(offset == 0, lines_to(shift), 0.0)
            stats = jnp.where(offset == LINES, lead, stats)
            stats = jnp.where(offset == 2 * LINES, lines_to(total) - lead, stats)
            stats = jnp.broadcast_to(jnp.sum(stats, axis=0, keepdims=True), (8, HD))
            whole = jnp.concatenate([lines_to(accum), stats], axis=0).astype(jnp.bfloat16)
            for far in range(FAR):
                out_ref[(half * FAR + far) * NEAR + near] = whole


def attention(queries, cache_keys, cache_values, new_keys, new_values, lengths, here):
    kinds = (queries, cache_keys, cache_values, new_keys, new_values)
    smem = pl.BlockSpec(memory_space=pltpu.SMEM)
    return pl.pallas_call(
        attend,
        out_shape=jax.ShapeDtypeStruct((2 * FAR * NEAR, LINES + 8, HD), jnp.bfloat16),
        in_specs=[smem, smem] + [pl.BlockSpec(memory_space=pl.ANY)] * 5,
        out_specs=pl.BlockSpec(memory_space=pltpu.VMEM),
        scratch_shapes=[pltpu.VMEM(a.shape, a.dtype) for a in kinds]
        + [pltpu.SemaphoreType.DMA((3,)), pltpu.SemaphoreType.DMA((2, queries.shape[0]))],
        cost_estimate=pl.CostEstimate(flops=10**8, bytes_accessed=1 << 20, transcendentals=1 << 15),
        name="attend",
    )(lengths, here, *kinds)


def layer(
    queries,
    cache_keys,
    cache_values,
    new_keys,
    new_values,
    lengths,
    residual,
    norm_gain,
    w_gate,
    w_down,
):
    rows, steps, features = queries.shape
    groups, halves = lax.axis_size(GRP), lax.axis_size("xh")
    tokens = rows * steps
    share = tokens // halves
    total_tokens = groups * tokens
    near, far = NEAR, FAR

    stacked = jnp.stack([w_gate.T, w_down.T]).astype(jnp.bfloat16)
    stacked = pad_to(stacked, 1, 2 * HALF).reshape(2, 2, HALF, HD)
    own, other = traded(stacked, 0), traded(stacked, 1)

    here = lax.axis_index(TP).reshape(1)
    sent = attention(queries, cache_keys, cache_values, new_keys, new_values, lengths, here)

    half, deep = lax.axis_index("xh"), lax.axis_index("z1")
    mine = residual.reshape(halves, share, 2, near, 4, HD)
    mine = lax.dynamic_index_in_dim(lax.dynamic_index_in_dim(mine, half, 0, False), deep, 2, False).astype(jnp.float32)
    gain = lax.dynamic_index_in_dim(norm_gain.reshape(2, near, 4, HD), deep, 1, False)
    pair = lax.axis_index("yb")
    own_gain = gain.reshape(2, 2, 2, HD)[lax.axis_index("xl"), :, lax.axis_index("c")]
    own_gain = jnp.where(pair == 0, own_gain, own_gain[::-1]).reshape(2 * HD)
    first = (lax.axis_index("z2") == 0).astype(jnp.float32)
    sent, mine, gain, own_gain, first = lax.optimization_barrier((sent, mine, gain, own_gain, first))
    pieces = exchange(sent, TP)

    stats = pieces[:, LINES, : 3 * LINES].astype(jnp.float32).reshape(-1, 3, LINES)
    joint = jnp.max(stats[:, 0], axis=0)
    factor = jnp.exp(stats[:, 0] - joint)
    total = jnp.sum(factor * (stats[:, 1] + stats[:, 2]), axis=0)
    context = jnp.sum(factor[..., None] * pieces[:, :LINES].astype(jnp.float32), axis=0) / total[:, None]
    context = jnp.transpose(context.reshape(rows // halves, 2, 4, steps, HD), (0, 3, 1, 2, 4))

    summed = mine + context.reshape(share, 2, 4, HD)
    gained = (summed * gain).astype(jnp.bfloat16).reshape(share, 2, 2, 2, HD)
    gained = jnp.transpose(gained, (1, 3, 0, 2, 4))
    ordered = jnp.stack([gained, gained[:, :, :, ::-1]], axis=1)
    ordered = jnp.broadcast_to(ordered[:, None, :, :, None], (2, near, 2, 2, halves, share, 2, HD))
    ordered = ordered.reshape(groups * halves, share, 2 * HD)
    kept = summed * first
    ordered, kept = lax.optimization_barrier((ordered, kept))
    arrived = exchange(ordered, WIDE)
    arrived = arrived.reshape(total_tokens, 2 * HD)

    unscaled = arrived.astype(jnp.float32) / own_gain
    squares = jnp.stack(two_words(jnp.sum(unscaled * unscaled, axis=-1)), axis=-1)
    turned = (((1,), (1,)), ((), ()))
    gate = lax.dot_general(arrived[:, :HD], own[0], turned, preferred_element_type=jnp.float32)
    gate = gate + lax.dot_general(arrived[:, HD:], other[0], turned, preferred_element_type=jnp.float32)
    sent = jnp.concatenate([gate.astype(jnp.bfloat16), squares], axis=-1)
    depth = lax.axis_size(DEEP)
    sums = exchange(sent.reshape(depth, total_tokens // depth, -1), DEEP).astype(jnp.float32).sum(axis=0)
    mean_square = (sums[:, HALF] + sums[:, HALF + 1]) / features
    gate = sums[:, :HALF] * lax.rsqrt(mean_square + 1e-05)[:, None]
    hidden = copies(jax.nn.silu(gate).astype(jnp.bfloat16), DEEP).reshape(total_tokens, HALF)
    terms = jnp.concatenate(
        [jnp.dot(hidden, w[1], preferred_element_type=jnp.float32).astype(jnp.bfloat16) for w in (own, other)], axis=-1
    )
    partial = exchange(terms.reshape(groups * halves, share, 2 * HD), WIDE)
    partial = partial.reshape(2, near, 2, 2, halves, share, 2, HD).astype(jnp.float32).sum(axis=(1, 4))
    mlp = partial[:, 0] + partial[:, 1, :, :, ::-1]
    mlp = jnp.transpose(mlp, (2, 0, 3, 1, 4)).reshape(share, 2, 4, HD)
    mixed = mlp + kept
    mixed = copies(mixed.astype(jnp.bfloat16).reshape(share, 8 * HD), TP)
    mixed = mixed.reshape(halves, far, near, share, 2, 4, HD).astype(jnp.float32).sum(axis=1)
    mixed = jnp.transpose(mixed, (0, 2, 3, 1, 4, 5))
    return mixed.astype(jnp.bfloat16).reshape(rows, steps, features)


def solution(mesh):
    fine = Mesh(mesh.devices.reshape(2, 4, 2, 2, 2, 3, 4), ("xl", "ya", "yb", "c", "xh", "z2", "z1"))
    return jax.shard_map(
        layer,
        mesh=fine,
        in_specs=(
            P(GRP, None, None),
            P(GRP, TP, None),
            P(GRP, TP, None),
            P(GRP, None, None),
            P(GRP, None, None),
            P(GRP),
            P(GRP, None, None),
            P(),
            P(GRP, TP),
            P(GRP, TP),
        ),
        out_specs=P(GRP, None, None),
        check_vma=False,
    )
```

```python
import jax
import jax.numpy as jnp
from jax import lax
from jax.experimental import pallas as pl
from jax.experimental.pallas import tpu as pltpu
from jax.sharding import Mesh
from jax.sharding import PartitionSpec as P


HD = 128
KVH = 4
HQ = 32
EACH = HQ // KVH
NEAR = 4
FAR = 3
LINES = 32
GRP = ("xl", "ya", "yb", "c")
TP = ("xh", "z2", "z1")
WIDE = ("xl", "ya", "yb", "c", "xh")
DEEP = ("xl", "c", "z1")
PIECE = 152
HALF = 2 * PIECE
masked_score = -1e30


def exchange(parts, axis):
    return lax.all_to_all(parts, axis, split_axis=0, concat_axis=0, tiled=True)


def copies(part, axis):
    return exchange(jnp.broadcast_to(part, (lax.axis_size(axis), *part.shape)), axis)


def two_words(value):
    high = value.astype(jnp.bfloat16)
    return high, (value - high.astype(jnp.float32)).astype(jnp.bfloat16)


def pad_to(array, axis, size):
    widths = [(0, 0)] * array.ndim
    widths[axis] = (0, size - array.shape[axis])
    return jnp.pad(array, widths)


def traded(pieces, turn):
    over, under = turn // 2, turn % 2
    moves = []
    for row in range(NEAR):
        for pair in range(2):
            for deep in range(NEAR):
                target = (pair ^ over) * 2 + (deep // 2 ^ under)
                moves.append(((row * 2 + pair) * NEAR + deep, (target * 2 + deep % 2) * NEAR + row))
    at = (lax.axis_index("yb") ^ over) * 2 + (lax.axis_index("z1") // 2 ^ under)
    sent = lax.dynamic_index_in_dim(pieces, at, 1, False)
    return lax.ppermute(sent, ("ya", "yb", "z1"), moves)


def attend(lengths_ref, here_ref, q_hbm, k_hbm, v_hbm, nk_hbm, nv_hbm, out_ref, q, k, v, nk, nv, small, large):
    rows, positions = k.shape[0], k.shape[1]
    pairs = ((q_hbm, q), (nk_hbm, nk), (nv_hbm, nv))
    first = [pltpu.make_async_copy(s, d, small.at[i]) for i, (s, d) in enumerate(pairs)]
    keys = [pltpu.make_async_copy(k_hbm.at[r], k.at[r], large.at[0, r]) for r in range(rows)]
    values = [pltpu.make_async_copy(v_hbm.at[r], v.at[r], large.at[1, r]) for r in range(rows)]
    for copy in first + keys + values:
        copy.start()
    here = here_ref[0]
    block = 2 * EACH
    lines = rows * KVH * block
    each_row = KVH * block
    step = lax.rem(lax.broadcasted_iota(jnp.int32, (lines, 1), 0), 2)
    fresh_ok = [(here == 0) & (step >= t) for t in range(2)]
    lane = lax.broadcasted_iota(jnp.int32, (each_row, positions), 1) + here * positions
    visible = jnp.concatenate([lane < lengths_ref[r] for r in range(rows)], axis=0)

    def all_lines(part):
        return jnp.concatenate([part(r, j) for r in range(rows) for j in range(KVH)], axis=0)

    def head_of(ref, r, j):
        return ref[r, :, j * HD : (j + 1) * HD]

    for copy in first:
        copy.wait()
    queries = []
    for r in range(rows):
        row = q[r].astype(jnp.float32)
        queries += [row[:, h * HD : (h + 1) * HD] for h in range(HQ)]
    queries = jnp.concatenate(queries, axis=0)
    narrow = queries.astype(jnp.bfloat16)

    def fresh_of(ref, t):
        return all_lines(
            lambda r, j: jnp.broadcast_to(ref[r, t : t + 1, j * HD : (j + 1) * HD].astype(jnp.float32), (block, HD))
        )

    fresh = [
        jnp.where(fresh_ok[t], jnp.sum(queries * fresh_of(nk, t), axis=1, keepdims=True) * HD**-0.5, masked_score)
        for t in range(2)
    ]
    for copy in keys:
        copy.wait()

    def lines_of(array, r, j):
        at = (r * KVH + j) * block
        return array[at : at + block]

    turned = (((1,), (1,)), ((), ()))
    scores = all_lines(
        lambda r, j: lax.dot_general(
            lines_of(narrow, r, j), head_of(k, r, j), turned, preferred_element_type=jnp.float32
        )
    )
    scores = jnp.where(visible, scores * HD**-0.5, masked_score)
    top = jnp.maximum(jnp.max(scores, axis=1, keepdims=True), jnp.maximum(*fresh))
    shift = top.astype(jnp.bfloat16).astype(jnp.float32)
    weights = jnp.where(visible, jnp.exp(scores - shift), 0.0)
    added = [jnp.where(fresh_ok[t], jnp.exp(fresh[t] - shift), 0.0) for t in range(2)]
    total = jnp.sum(weights, axis=1, keepdims=True) + added[0] + added[1]
    weights = weights.astype(jnp.bfloat16)
    for copy in values:
        copy.wait()
    accum = all_lines(
        lambda r, j: jnp.dot(lines_of(weights, r, j), head_of(v, r, j), preferred_element_type=jnp.float32)
    )
    for t in range(2):
        accum += added[t].astype(jnp.bfloat16).astype(jnp.float32) * fresh_of(nv, t)
    high = total.astype(jnp.bfloat16).astype(jnp.float32)
    line = lax.broadcasted_iota(jnp.int32, (LINES, HD), 0)
    offset = lax.broadcasted_iota(jnp.int32, (LINES, HD), 1) - line
    for half in range(2):
        for near in range(NEAR):

            def lines_to(array):
                parts = []
                for r in range(half * rows // 2, (half + 1) * rows // 2):
                    for side in range(2):
                        at = (r * KVH + side * 2 + near // 2) * block + near % 2 * 8
                        parts.append(array[at : at + 8])
                return jnp.concatenate(parts, axis=0)

            lead = lines_to(high)
            stats = jnp.where(offset == 0, lines_to(shift), 0.0)
            stats = jnp.where(offset == LINES, lead, stats)
            stats = jnp.where(offset == 2 * LINES, lines_to(total) - lead, stats)
            stats = jnp.broadcast_to(jnp.sum(stats, axis=0, keepdims=True), (8, HD))
            whole = jnp.concatenate([lines_to(accum), stats], axis=0).astype(jnp.bfloat16)
            for far in range(FAR):
                out_ref[(half * FAR + far) * NEAR + near] = whole


def attention(queries, cache_keys, cache_values, new_keys, new_values, lengths, here):
    kinds = (queries, cache_keys, cache_values, new_keys, new_values)
    smem = pl.BlockSpec(memory_space=pltpu.SMEM)
    return pl.pallas_call(
        attend,
        out_shape=jax.ShapeDtypeStruct((2 * FAR * NEAR, LINES + 8, HD), jnp.bfloat16),
        in_specs=[smem, smem] + [pl.BlockSpec(memory_space=pl.ANY)] * 5,
        out_specs=pl.BlockSpec(memory_space=pltpu.VMEM),
        scratch_shapes=[pltpu.VMEM(a.shape, a.dtype) for a in kinds]
        + [pltpu.SemaphoreType.DMA((3,)), pltpu.SemaphoreType.DMA((2, queries.shape[0]))],
        cost_estimate=pl.CostEstimate(flops=10**8, bytes_accessed=1 << 20, transcendentals=1 << 15),
        name="attend",
    )(lengths, here, *kinds)


def layer(
    queries,
    cache_keys,
    cache_values,
    new_keys,
    new_values,
    lengths,
    residual,
    norm_gain,
    w_gate,
    w_down,
):
    rows, steps, features = queries.shape
    groups, halves = lax.axis_size(GRP), lax.axis_size("xh")
    tokens = rows * steps
    share = tokens // halves
    total_tokens = groups * tokens
    near, far = NEAR, FAR

    stacked = jnp.stack([w_gate.T, w_down.T]).astype(jnp.bfloat16)
    stacked = pad_to(stacked, 1, 4 * PIECE).reshape(2, 4, PIECE, HD)
    moved = [traded(stacked, turn) for turn in range(4)]

    here = lax.axis_index(TP).reshape(1)
    sent = attention(queries, cache_keys, cache_values, new_keys, new_values, lengths, here)

    half, deep = lax.axis_index("xh"), lax.axis_index("z1")
    mine = residual.reshape(halves, share, 2, near, 4, HD)
    mine = lax.dynamic_index_in_dim(lax.dynamic_index_in_dim(mine, half, 0, False), deep, 2, False).astype(jnp.float32)
    gain = lax.dynamic_index_in_dim(norm_gain.reshape(2, near, 4, HD), deep, 1, False)
    own_gain = gain.reshape(2, 2, 2, HD)[lax.axis_index("xl"), :, lax.axis_index("c")]
    own_gain = jnp.where(lax.axis_index("ya") < NEAR // 2, own_gain, own_gain[::-1]).reshape(2 * HD)
    first = (lax.axis_index("z2") == 0).astype(jnp.float32)
    pieces = exchange(sent, TP)

    stats = pieces[:, LINES, : 3 * LINES].astype(jnp.float32).reshape(-1, 3, LINES)
    joint = jnp.max(stats[:, 0], axis=0)
    factor = jnp.exp(stats[:, 0] - joint)
    total = jnp.sum(factor * (stats[:, 1] + stats[:, 2]), axis=0)
    context = jnp.sum(factor[..., None] * pieces[:, :LINES].astype(jnp.float32), axis=0) / total[:, None]
    context = jnp.transpose(context.reshape(rows // halves, 2, 4, steps, HD), (0, 3, 1, 2, 4))

    summed = mine + context.reshape(share, 2, 4, HD)
    gained = (summed * gain).astype(jnp.bfloat16).reshape(share, 2, 2, 2, HD)
    gained = jnp.transpose(gained, (1, 3, 0, 2, 4))
    ordered = jnp.stack([gained, gained[:, :, :, ::-1]], axis=1)
    ordered = jnp.broadcast_to(ordered[:, :, None, :, None], (2, 2, near, 2, halves, share, 2, HD))
    ordered = ordered.reshape(groups * halves, share, 2 * HD)
    kept = summed * first
    ordered, kept, own_gain = lax.optimization_barrier((ordered, kept, own_gain))
    arrived = exchange(ordered, WIDE)
    arrived = arrived.reshape(total_tokens, 2 * HD)

    unscaled = arrived.astype(jnp.float32) / own_gain
    squares = jnp.stack(two_words(jnp.sum(unscaled * unscaled, axis=-1)), axis=-1)
    squares, moved = lax.optimization_barrier((squares, moved))
    turned = (((1,), (1,)), ((), ()))
    gate_weights, down_weights = (
        [jnp.concatenate([moved[2 * block][kind], moved[2 * block + 1][kind]], axis=0) for block in range(2)]
        for kind in range(2)
    )
    gate = sum(
        lax.dot_general(arrived[:, at * HD : (at + 1) * HD], w, turned, preferred_element_type=jnp.float32)
        for at, w in enumerate(gate_weights)
    )
    sent = jnp.concatenate([gate.astype(jnp.bfloat16), squares], axis=-1)
    depth = lax.axis_size(DEEP)
    sums = exchange(sent.reshape(depth, total_tokens // depth, -1), DEEP).astype(jnp.float32).sum(axis=0)
    mean_square = (sums[:, HALF] + sums[:, HALF + 1]) / features
    gate = sums[:, :HALF] * lax.rsqrt(mean_square + 1e-05)[:, None]
    hidden = copies(jax.nn.silu(gate).astype(jnp.bfloat16), DEEP).reshape(total_tokens, HALF)
    terms = jnp.concatenate(
        [jnp.dot(hidden, w, preferred_element_type=jnp.float32).astype(jnp.bfloat16) for w in down_weights], axis=-1
    )
    partial = exchange(terms.reshape(groups * halves, share, 2 * HD), WIDE)
    partial = partial.reshape(2, 2, near, 2, halves, share, 2, HD).astype(jnp.float32).sum(axis=(2, 4))
    mlp = partial[:, 0] + partial[:, 1, :, :, ::-1]
    mlp = jnp.transpose(mlp, (2, 0, 3, 1, 4)).reshape(share, 2, 4, HD)
    mixed = mlp + kept
    mixed = copies(mixed.astype(jnp.bfloat16).reshape(share, 8 * HD), TP)
    mixed = mixed.reshape(halves, far, near, share, 2, 4, HD).astype(jnp.float32).sum(axis=1)
    mixed = jnp.transpose(mixed, (0, 2, 3, 1, 4, 5))
    return mixed.astype(jnp.bfloat16).reshape(rows, steps, features)


def solution(mesh):
    fine = Mesh(mesh.devices.reshape(2, 4, 2, 2, 2, 3, 4), ("xl", "ya", "yb", "c", "xh", "z2", "z1"))
    return jax.shard_map(
        layer,
        mesh=fine,
        in_specs=(
            P(GRP, None, None),
            P(GRP, TP, None),
            P(GRP, TP, None),
            P(GRP, None, None),
            P(GRP, None, None),
            P(GRP),
            P(GRP, None, None),
            P(),
            P(GRP, TP),
            P(GRP, TP),
        ),
        out_specs=P(GRP, None, None),
        check_vma=False,
    )
```

```python
import jax
import jax.numpy as jnp
from jax import lax
from jax.experimental import pallas as pl
from jax.experimental.pallas import tpu as pltpu
from jax.sharding import Mesh
from jax.sharding import PartitionSpec as P


HD = 128
KVH = 4
HQ = 32
EACH = HQ // KVH
NEAR = 4
FAR = 3
LINES = 32
GRP = ("xl", "ya", "yb", "c")
TP = ("xh", "z2", "z1")
WIDE = ("xl", "ya", "yb", "c", "xh")
DEEP = ("xl", "c", "z1")
HALF = 304
masked_score = -1e30


def exchange(parts, axis):
    return lax.all_to_all(parts, axis, split_axis=0, concat_axis=0, tiled=True)


def copies(part, axis):
    return exchange(jnp.broadcast_to(part, (lax.axis_size(axis), *part.shape)), axis)


def two_words(value):
    high = value.astype(jnp.bfloat16)
    return high, (value - high.astype(jnp.float32)).astype(jnp.bfloat16)


def pad_to(array, axis, size):
    widths = [(0, 0)] * array.ndim
    widths[axis] = (0, size - array.shape[axis])
    return jnp.pad(array, widths)


def traded(halves, turn):
    moves = []
    for row in range(NEAR):
        for pair in range(2):
            for deep in range(NEAR):
                target = (pair ^ turn) * NEAR + deep
                moves.append(((row * 2 + pair) * NEAR + deep, target * NEAR + row))
    sent = lax.dynamic_index_in_dim(halves, lax.axis_index("yb") ^ turn, 0, False)
    return lax.ppermute(sent, ("ya", "yb", "z1"), moves)


def attend(lengths_ref, here_ref, q_hbm, k_hbm, v_hbm, nk_hbm, nv_hbm, out_ref, q, k, v, nk, nv, small, large):
    rows, positions = k.shape[0], k.shape[1]
    pairs = ((q_hbm, q), (nk_hbm, nk), (nv_hbm, nv))
    first = [pltpu.make_async_copy(s, d, small.at[i]) for i, (s, d) in enumerate(pairs)]
    keys = [pltpu.make_async_copy(k_hbm.at[r], k.at[r], large.at[0, r]) for r in range(rows)]
    values = [pltpu.make_async_copy(v_hbm.at[r], v.at[r], large.at[1, r]) for r in range(rows)]
    for copy in first + keys + values:
        copy.start()
    here = here_ref[0]
    block = 2 * EACH
    lines = rows * KVH * block
    each_row = KVH * block
    step = lax.rem(lax.broadcasted_iota(jnp.int32, (lines, 1), 0), 2)
    fresh_ok = [(here == 0) & (step >= t) for t in range(2)]
    lane = lax.broadcasted_iota(jnp.int32, (each_row, positions), 1) + here * positions
    visible = jnp.concatenate([lane < lengths_ref[r] for r in range(rows)], axis=0)

    def all_lines(part):
        return jnp.concatenate([part(r, j) for r in range(rows) for j in range(KVH)], axis=0)

    def head_of(ref, r, j):
        return ref[r, :, j * HD : (j + 1) * HD]

    for copy in first:
        copy.wait()
    queries = []
    for r in range(rows):
        row = q[r].astype(jnp.float32)
        queries += [row[:, h * HD : (h + 1) * HD] for h in range(HQ)]
    queries = jnp.concatenate(queries, axis=0)
    narrow = queries.astype(jnp.bfloat16)

    def fresh_of(ref, t):
        return all_lines(
            lambda r, j: jnp.broadcast_to(ref[r, t : t + 1, j * HD : (j + 1) * HD].astype(jnp.float32), (block, HD))
        )

    fresh = [
        jnp.where(fresh_ok[t], jnp.sum(queries * fresh_of(nk, t), axis=1, keepdims=True) * HD**-0.5, masked_score)
        for t in range(2)
    ]
    for copy in keys:
        copy.wait()

    def lines_of(array, r, j):
        at = (r * KVH + j) * block
        return array[at : at + block]

    turned = (((1,), (1,)), ((), ()))
    scores = all_lines(
        lambda r, j: lax.dot_general(
            lines_of(narrow, r, j), head_of(k, r, j), turned, preferred_element_type=jnp.float32
        )
    )
    scores = jnp.where(visible, scores * HD**-0.5, masked_score)
    top = jnp.maximum(jnp.max(scores, axis=1, keepdims=True), jnp.maximum(*fresh))
    shift = top.astype(jnp.bfloat16).astype(jnp.float32)
    weights = jnp.where(visible, jnp.exp(scores - shift), 0.0)
    added = [jnp.where(fresh_ok[t], jnp.exp(fresh[t] - shift), 0.0) for t in range(2)]
    total = jnp.sum(weights, axis=1, keepdims=True) + added[0] + added[1]
    weights = weights.astype(jnp.bfloat16)
    for copy in values:
        copy.wait()
    accum = all_lines(
        lambda r, j: jnp.dot(lines_of(weights, r, j), head_of(v, r, j), preferred_element_type=jnp.float32)
    )
    for t in range(2):
        accum += added[t].astype(jnp.bfloat16).astype(jnp.float32) * fresh_of(nv, t)
    high = total.astype(jnp.bfloat16).astype(jnp.float32)
    line = lax.broadcasted_iota(jnp.int32, (LINES, HD), 0)
    offset = lax.broadcasted_iota(jnp.int32, (LINES, HD), 1) - line
    for half in range(2):
        for near in range(NEAR):

            def lines_to(array):
                parts = []
                for r in range(half * rows // 2, (half + 1) * rows // 2):
                    for side in range(2):
                        at = (r * KVH + side * 2 + near // 2) * block + near % 2 * 8
                        parts.append(array[at : at + 8])
                return jnp.concatenate(parts, axis=0)

            lead = lines_to(high)
            stats = jnp.where(offset == 0, lines_to(shift), 0.0)
            stats = jnp.where(offset == LINES, lead, stats)
            stats = jnp.where(offset == 2 * LINES, lines_to(total) - lead, stats)
            stats = jnp.broadcast_to(jnp.sum(stats, axis=0, keepdims=True), (8, HD))
            whole = jnp.concatenate([lines_to(accum), stats], axis=0).astype(jnp.bfloat16)
            for far in range(FAR):
                out_ref[(half * FAR + far) * NEAR + near] = whole


def attention(queries, cache_keys, cache_values, new_keys, new_values, lengths, here):
    kinds = (queries, cache_keys, cache_values, new_keys, new_values)
    smem = pl.BlockSpec(memory_space=pltpu.SMEM)
    return pl.pallas_call(
        attend,
        out_shape=jax.ShapeDtypeStruct((2 * FAR * NEAR, LINES + 8, HD), jnp.bfloat16),
        in_specs=[smem, smem] + [pl.BlockSpec(memory_space=pl.ANY)] * 5,
        out_specs=pl.BlockSpec(memory_space=pltpu.VMEM),
        scratch_shapes=[pltpu.VMEM(a.shape, a.dtype) for a in kinds]
        + [pltpu.SemaphoreType.DMA((3,)), pltpu.SemaphoreType.DMA((2, queries.shape[0]))],
        cost_estimate=pl.CostEstimate(flops=10**8, bytes_accessed=1 << 20, transcendentals=1 << 15),
        name="attend",
    )(lengths, here, *kinds)


def layer(
    queries,
    cache_keys,
    cache_values,
    new_keys,
    new_values,
    lengths,
    residual,
    norm_gain,
    w_gate,
    w_down,
):
    rows, steps, features = queries.shape
    groups, halves = lax.axis_size(GRP), lax.axis_size("xh")
    tokens = rows * steps
    share = tokens // halves
    total_tokens = groups * tokens
    near, far = NEAR, FAR

    def moved(weights):
        halves = pad_to(weights.T.astype(jnp.bfloat16), 0, 2 * HALF).reshape(2, HALF, HD)
        return [traded(halves, turn) for turn in range(2)]

    gate_weights, down_weights = moved(w_gate), moved(w_down)

    here = lax.axis_index(TP).reshape(1)
    sent = attention(queries, cache_keys, cache_values, new_keys, new_values, lengths, here)

    half, deep = lax.axis_index("xh"), lax.axis_index("z1")
    mine = residual.reshape(halves, share, 2, near, 4, HD)
    mine = lax.dynamic_index_in_dim(lax.dynamic_index_in_dim(mine, half, 0, False), deep, 2, False).astype(jnp.float32)
    gain = lax.dynamic_index_in_dim(norm_gain.reshape(2, near, 4, HD), deep, 1, False)
    own_gain = gain.reshape(2, 2, 2, HD)[lax.axis_index("xl"), :, lax.axis_index("c")]
    own_gain = jnp.where(lax.axis_index("ya") < NEAR // 2, own_gain, own_gain[::-1]).reshape(2 * HD)
    first = (lax.axis_index("z2") == 0).astype(jnp.float32)
    pieces = exchange(sent, TP)

    stats = pieces[:, LINES, : 3 * LINES].astype(jnp.float32).reshape(-1, 3, LINES)
    joint = jnp.max(stats[:, 0], axis=0)
    factor = jnp.exp(stats[:, 0] - joint)
    total = jnp.sum(factor * (stats[:, 1] + stats[:, 2]), axis=0)
    context = jnp.sum(factor[..., None] * pieces[:, :LINES].astype(jnp.float32), axis=0) / total[:, None]
    context = jnp.transpose(context.reshape(rows // halves, 2, 4, steps, HD), (0, 3, 1, 2, 4))

    summed = mine + context.reshape(share, 2, 4, HD)
    gained = (summed * gain).astype(jnp.bfloat16).reshape(share, 2, 2, 2, HD)
    gained = jnp.transpose(gained, (1, 3, 0, 2, 4))
    ordered = jnp.stack([gained, gained[:, :, :, ::-1]], axis=1)
    ordered = jnp.broadcast_to(ordered[:, :, None, :, None], (2, 2, near, 2, halves, share, 2, HD))
    ordered = ordered.reshape(groups * halves, share, 2 * HD)
    kept = summed * first
    ordered, kept, own_gain = lax.optimization_barrier((ordered, kept, own_gain))
    arrived = exchange(ordered, WIDE)
    arrived = arrived.reshape(total_tokens, 2 * HD)

    unscaled = arrived.astype(jnp.float32) / own_gain
    squares = jnp.stack(two_words(jnp.sum(unscaled * unscaled, axis=-1)), axis=-1)
    turned = (((1,), (1,)), ((), ()))
    gate = sum(
        lax.dot_general(arrived[:, at * HD : (at + 1) * HD], w, turned, preferred_element_type=jnp.float32)
        for at, w in enumerate(gate_weights)
    )
    sent = jnp.concatenate([gate.astype(jnp.bfloat16), squares], axis=-1)
    depth = lax.axis_size(DEEP)
    sums = exchange(sent.reshape(depth, total_tokens // depth, -1), DEEP).astype(jnp.float32).sum(axis=0)
    mean_square = (sums[:, HALF] + sums[:, HALF + 1]) / features
    gate = sums[:, :HALF] * lax.rsqrt(mean_square + 1e-05)[:, None]
    hidden = jax.nn.silu(gate).astype(jnp.bfloat16)
    hidden, down_weights = lax.optimization_barrier((hidden, down_weights))
    hidden = copies(hidden, DEEP).reshape(total_tokens, HALF)
    terms = jnp.concatenate(
        [jnp.dot(hidden, w, preferred_element_type=jnp.float32).astype(jnp.bfloat16) for w in down_weights], axis=-1
    )
    partial = exchange(terms.reshape(groups * halves, share, 2 * HD), WIDE)
    partial = partial.reshape(2, 2, near, 2, halves, share, 2, HD).astype(jnp.float32).sum(axis=(2, 4))
    mlp = partial[:, 0] + partial[:, 1, :, :, ::-1]
    mlp = jnp.transpose(mlp, (2, 0, 3, 1, 4)).reshape(share, 2, 4, HD)
    mixed = mlp + kept
    mixed = copies(mixed.astype(jnp.bfloat16).reshape(share, 8 * HD), TP)
    mixed = mixed.reshape(halves, far, near, share, 2, 4, HD).astype(jnp.float32).sum(axis=1)
    mixed = jnp.transpose(mixed, (0, 2, 3, 1, 4, 5))
    return mixed.astype(jnp.bfloat16).reshape(rows, steps, features)


def solution(mesh):
    fine = Mesh(mesh.devices.reshape(2, 4, 2, 2, 2, 3, 4), ("xl", "ya", "yb", "c", "xh", "z2", "z1"))
    return jax.shard_map(
        layer,
        mesh=fine,
        in_specs=(
            P(GRP, None, None),
            P(GRP, TP, None),
            P(GRP, TP, None),
            P(GRP, None, None),
            P(GRP, None, None),
            P(GRP),
            P(GRP, None, None),
            P(),
            P(GRP, TP),
            P(GRP, TP),
        ),
        out_specs=P(GRP, None, None),
        check_vma=False,
    )
```

```python
import jax
import jax.numpy as jnp
from jax import lax
from jax.experimental import pallas as pl
from jax.experimental.pallas import tpu as pltpu
from jax.sharding import Mesh
from jax.sharding import PartitionSpec as P


HD = 128
KVH = 4
HQ = 32
EACH = HQ // KVH
NEAR = 4
FAR = 3
LINES = 32
GRP = ("xl", "ya", "yb", "c")
TP = ("xh", "z2", "z1")
WIDE = ("xl", "ya", "yb", "c", "xh")
DEEP = ("xl", "c", "z1")
HALF = 304
masked_score = -1e30


def exchange(parts, axis):
    return lax.all_to_all(parts, axis, split_axis=0, concat_axis=0, tiled=True)


def copies(part, axis):
    return exchange(jnp.broadcast_to(part, (lax.axis_size(axis), *part.shape)), axis)


def two_words(value):
    high = value.astype(jnp.bfloat16)
    return high, (value - high.astype(jnp.float32)).astype(jnp.bfloat16)


def pad_to(array, axis, size):
    widths = [(0, 0)] * array.ndim
    widths[axis] = (0, size - array.shape[axis])
    return jnp.pad(array, widths)


def traded(halves, turn):
    moves = []
    for row in range(NEAR):
        for pair in range(2):
            for deep in range(NEAR):
                target = (pair ^ turn) * NEAR + deep
                moves.append(((row * 2 + pair) * NEAR + deep, target * NEAR + row))
    sent = lax.dynamic_index_in_dim(halves, lax.axis_index("yb") ^ turn, 1, False)
    return lax.ppermute(sent, ("ya", "yb", "z1"), moves)


def attend(lengths_ref, here_ref, q_hbm, k_hbm, v_hbm, nk_hbm, nv_hbm, out_ref, q, k, v, nk, nv, small, large):
    rows, positions = k.shape[0], k.shape[1]
    pairs = ((q_hbm, q), (nk_hbm, nk), (nv_hbm, nv))
    first = [pltpu.make_async_copy(s, d, small.at[i]) for i, (s, d) in enumerate(pairs)]
    keys = [pltpu.make_async_copy(k_hbm.at[r], k.at[r], large.at[0, r]) for r in range(rows)]
    values = [pltpu.make_async_copy(v_hbm.at[r], v.at[r], large.at[1, r]) for r in range(rows)]
    for copy in first + keys + values:
        copy.start()
    here = here_ref[0]
    block = 2 * EACH
    lines = rows * KVH * block
    each_row = KVH * block
    step = lax.rem(lax.broadcasted_iota(jnp.int32, (lines, 1), 0), 2)
    fresh_ok = [(here == 0) & (step >= t) for t in range(2)]
    lane = lax.broadcasted_iota(jnp.int32, (each_row, positions), 1) + here * positions
    visible = jnp.concatenate([lane < lengths_ref[r] for r in range(rows)], axis=0)

    def all_lines(part):
        return jnp.concatenate([part(r, j) for r in range(rows) for j in range(KVH)], axis=0)

    def head_of(ref, r, j):
        return ref[r, :, j * HD : (j + 1) * HD]

    for copy in first:
        copy.wait()
    queries = []
    for r in range(rows):
        row = q[r].astype(jnp.float32)
        queries += [row[:, h * HD : (h + 1) * HD] for h in range(HQ)]
    queries = jnp.concatenate(queries, axis=0)
    narrow = queries.astype(jnp.bfloat16)

    def fresh_of(ref, t):
        return all_lines(
            lambda r, j: jnp.broadcast_to(ref[r, t : t + 1, j * HD : (j + 1) * HD].astype(jnp.float32), (block, HD))
        )

    fresh = [
        jnp.where(fresh_ok[t], jnp.sum(queries * fresh_of(nk, t), axis=1, keepdims=True) * HD**-0.5, masked_score)
        for t in range(2)
    ]
    for copy in keys:
        copy.wait()

    def lines_of(array, r, j):
        at = (r * KVH + j) * block
        return array[at : at + block]

    turned = (((1,), (1,)), ((), ()))
    scores = all_lines(
        lambda r, j: lax.dot_general(
            lines_of(narrow, r, j), head_of(k, r, j), turned, preferred_element_type=jnp.float32
        )
    )
    scores = jnp.where(visible, scores * HD**-0.5, masked_score)
    top = jnp.maximum(jnp.max(scores, axis=1, keepdims=True), jnp.maximum(*fresh))
    shift = top.astype(jnp.bfloat16).astype(jnp.float32)
    weights = jnp.where(visible, jnp.exp(scores - shift), 0.0)
    added = [jnp.where(fresh_ok[t], jnp.exp(fresh[t] - shift), 0.0) for t in range(2)]
    total = jnp.sum(weights, axis=1, keepdims=True) + added[0] + added[1]
    weights = weights.astype(jnp.bfloat16)
    for copy in values:
        copy.wait()
    accum = all_lines(
        lambda r, j: jnp.dot(lines_of(weights, r, j), head_of(v, r, j), preferred_element_type=jnp.float32)
    )
    for t in range(2):
        accum += added[t].astype(jnp.bfloat16).astype(jnp.float32) * fresh_of(nv, t)
    high = total.astype(jnp.bfloat16).astype(jnp.float32)
    line = lax.broadcasted_iota(jnp.int32, (LINES, HD), 0)
    offset = lax.broadcasted_iota(jnp.int32, (LINES, HD), 1) - line
    for half in range(2):
        for near in range(NEAR):

            def lines_to(array):
                parts = []
                for r in range(half * rows // 2, (half + 1) * rows // 2):
                    for side in range(2):
                        at = (r * KVH + side * 2 + near // 2) * block + near % 2 * 8
                        parts.append(array[at : at + 8])
                return jnp.concatenate(parts, axis=0)

            lead = lines_to(high)
            stats = jnp.where(offset == 0, lines_to(shift), 0.0)
            stats = jnp.where(offset == LINES, lead, stats)
            stats = jnp.where(offset == 2 * LINES, lines_to(total) - lead, stats)
            stats = jnp.broadcast_to(jnp.sum(stats, axis=0, keepdims=True), (8, HD))
            whole = jnp.concatenate([lines_to(accum), stats], axis=0).astype(jnp.bfloat16)
            for far in range(FAR):
                out_ref[(half * FAR + far) * NEAR + near] = whole


def attention(queries, cache_keys, cache_values, new_keys, new_values, lengths, here):
    kinds = (queries, cache_keys, cache_values, new_keys, new_values)
    smem = pl.BlockSpec(memory_space=pltpu.SMEM)
    return pl.pallas_call(
        attend,
        out_shape=jax.ShapeDtypeStruct((2 * FAR * NEAR, LINES + 8, HD), jnp.bfloat16),
        in_specs=[smem, smem] + [pl.BlockSpec(memory_space=pl.ANY)] * 5,
        out_specs=pl.BlockSpec(memory_space=pltpu.VMEM),
        scratch_shapes=[pltpu.VMEM(a.shape, a.dtype) for a in kinds]
        + [pltpu.SemaphoreType.DMA((3,)), pltpu.SemaphoreType.DMA((2, queries.shape[0]))],
        cost_estimate=pl.CostEstimate(flops=10**8, bytes_accessed=1 << 20, transcendentals=1 << 15),
        name="attend",
    )(lengths, here, *kinds)


def layer(
    queries,
    cache_keys,
    cache_values,
    new_keys,
    new_values,
    lengths,
    residual,
    norm_gain,
    w_gate,
    w_down,
):
    rows, steps, features = queries.shape
    groups, halves = lax.axis_size(GRP), lax.axis_size("xh")
    tokens = rows * steps
    share = tokens // halves
    total_tokens = groups * tokens
    near, far = NEAR, FAR

    stacked = jnp.stack([w_gate.T, w_down.T]).astype(jnp.bfloat16)
    halves_of = pad_to(stacked, 1, 2 * HALF).reshape(2, 2, HALF, HD)
    moved = [traded(halves_of, turn) for turn in range(2)]
    gate_weights, down_weights = ([pieces[kind] for pieces in moved] for kind in range(2))

    here = lax.axis_index(TP).reshape(1)
    sent = attention(queries, cache_keys, cache_values, new_keys, new_values, lengths, here)

    half, deep = lax.axis_index("xh"), lax.axis_index("z1")
    mine = residual.reshape(halves, share, 2, near, 4, HD)
    mine = lax.dynamic_index_in_dim(lax.dynamic_index_in_dim(mine, half, 0, False), deep, 2, False).astype(jnp.float32)
    gain = lax.dynamic_index_in_dim(norm_gain.reshape(2, near, 4, HD), deep, 1, False)
    own_gain = gain.reshape(2, 2, 2, HD)[lax.axis_index("xl"), :, lax.axis_index("c")]
    own_gain = jnp.where(lax.axis_index("ya") < NEAR // 2, own_gain, own_gain[::-1]).reshape(2 * HD)
    first = (lax.axis_index("z2") == 0).astype(jnp.float32)
    pieces = exchange(sent, TP)

    stats = pieces[:, LINES, : 3 * LINES].astype(jnp.float32).reshape(-1, 3, LINES)
    joint = jnp.max(stats[:, 0], axis=0)
    factor = jnp.exp(stats[:, 0] - joint)
    total = jnp.sum(factor * (stats[:, 1] + stats[:, 2]), axis=0)
    context = jnp.sum(factor[..., None] * pieces[:, :LINES].astype(jnp.float32), axis=0) / total[:, None]
    context = jnp.transpose(context.reshape(rows // halves, 2, 4, steps, HD), (0, 3, 1, 2, 4))

    summed = mine + context.reshape(share, 2, 4, HD)
    gained = (summed * gain).astype(jnp.bfloat16).reshape(share, 2, 2, 2, HD)
    gained = jnp.transpose(gained, (1, 3, 0, 2, 4))
    ordered = jnp.stack([gained, gained[:, :, :, ::-1]], axis=1)
    ordered = jnp.broadcast_to(ordered[:, :, None, :, None], (2, 2, near, 2, halves, share, 2, HD))
    ordered = ordered.reshape(groups * halves, share, 2 * HD)
    kept = summed * first
    ordered, kept, own_gain = lax.optimization_barrier((ordered, kept, own_gain))
    arrived = exchange(ordered, WIDE)
    arrived = arrived.reshape(total_tokens, 2 * HD)

    unscaled = arrived.astype(jnp.float32) / own_gain
    squares = jnp.stack(two_words(jnp.sum(unscaled * unscaled, axis=-1)), axis=-1)
    turned = (((1,), (1,)), ((), ()))
    gate = sum(
        lax.dot_general(arrived[:, at * HD : (at + 1) * HD], w, turned, preferred_element_type=jnp.float32)
        for at, w in enumerate(gate_weights)
    )
    sent = jnp.concatenate([gate.astype(jnp.bfloat16), squares], axis=-1)
    depth = lax.axis_size(DEEP)
    sums = exchange(sent.reshape(depth, total_tokens // depth, -1), DEEP).astype(jnp.float32).sum(axis=0)
    mean_square = (sums[:, HALF] + sums[:, HALF + 1]) / features
    gate = sums[:, :HALF] * lax.rsqrt(mean_square + 1e-05)[:, None]
    hidden = jax.nn.silu(gate).astype(jnp.bfloat16)
    hidden = copies(hidden, DEEP).reshape(total_tokens, HALF)
    terms = jnp.concatenate(
        [jnp.dot(hidden, w, preferred_element_type=jnp.float32).astype(jnp.bfloat16) for w in down_weights], axis=-1
    )
    partial = exchange(terms.reshape(groups * halves, share, 2 * HD), WIDE)
    partial = partial.reshape(2, 2, near, 2, halves, share, 2, HD).astype(jnp.float32).sum(axis=(2, 4))
    mlp = partial[:, 0] + partial[:, 1, :, :, ::-1]
    mlp = jnp.transpose(mlp, (2, 0, 3, 1, 4)).reshape(share, 2, 4, HD)
    mixed = mlp + kept
    mixed = copies(mixed.astype(jnp.bfloat16).reshape(share, 8 * HD), TP)
    mixed = mixed.reshape(halves, far, near, share, 2, 4, HD).astype(jnp.float32).sum(axis=1)
    mixed = jnp.transpose(mixed, (0, 2, 3, 1, 4, 5))
    return mixed.astype(jnp.bfloat16).reshape(rows, steps, features)


def solution(mesh):
    fine = Mesh(mesh.devices.reshape(2, 4, 2, 2, 2, 3, 4), ("xl", "ya", "yb", "c", "xh", "z2", "z1"))
    return jax.shard_map(
        layer,
        mesh=fine,
        in_specs=(
            P(GRP, None, None),
            P(GRP, TP, None),
            P(GRP, TP, None),
            P(GRP, None, None),
            P(GRP, None, None),
            P(GRP),
            P(GRP, None, None),
            P(),
            P(GRP, TP),
            P(GRP, TP),
        ),
        out_specs=P(GRP, None, None),
        check_vma=False,
    )
```

```python
import jax
import jax.numpy as jnp
from jax import lax
from jax.experimental import pallas as pl
from jax.experimental.pallas import tpu as pltpu
from jax.sharding import Mesh
from jax.sharding import PartitionSpec as P


HD = 128
KVH = 4
HQ = 32
EACH = HQ // KVH
NEAR = 4
FAR = 3
LINES = 32
GRP = ("xl", "ya", "yb", "c")
TP = ("xh", "z2", "z1")
WIDE = ("xl", "ya", "yb", "c", "xh")
DEEP = ("xl", "c", "z1")
HALF = 304
masked_score = -1e30


def exchange(parts, axis):
    return lax.all_to_all(parts, axis, split_axis=0, concat_axis=0, tiled=True)


def copies(part, axis):
    return exchange(jnp.broadcast_to(part, (lax.axis_size(axis), *part.shape)), axis)


def two_words(value):
    high = value.astype(jnp.bfloat16)
    return high, (value - high.astype(jnp.float32)).astype(jnp.bfloat16)


def pad_to(array, axis, size):
    widths = [(0, 0)] * array.ndim
    widths[axis] = (0, size - array.shape[axis])
    return jnp.pad(array, widths)


def traded(halves, turn):
    moves = []
    for row in range(NEAR):
        for pair in range(2):
            for deep in range(NEAR):
                target = (pair ^ turn) * NEAR + deep
                moves.append(((row * 2 + pair) * NEAR + deep, target * NEAR + row))
    sent = lax.dynamic_index_in_dim(halves, lax.axis_index("yb") ^ turn, 0, False)
    return lax.ppermute(sent, ("ya", "yb", "z1"), moves)


def attend(lengths_ref, here_ref, q_hbm, k_hbm, v_hbm, nk_hbm, nv_hbm, out_ref, q, k, v, nk, nv, small, large):
    rows, positions = k.shape[0], k.shape[1]
    pairs = ((q_hbm, q), (nk_hbm, nk), (nv_hbm, nv))
    first = [pltpu.make_async_copy(s, d, small.at[i]) for i, (s, d) in enumerate(pairs)]
    keys = [pltpu.make_async_copy(k_hbm.at[r], k.at[r], large.at[0, r]) for r in range(rows)]
    values = [pltpu.make_async_copy(v_hbm.at[r], v.at[r], large.at[1, r]) for r in range(rows)]
    for copy in first + keys + values:
        copy.start()
    here = here_ref[0]
    block = 2 * EACH
    lines = rows * KVH * block
    each_row = KVH * block
    step = lax.rem(lax.broadcasted_iota(jnp.int32, (lines, 1), 0), 2)
    fresh_ok = [(here == 0) & (step >= t) for t in range(2)]
    lane = lax.broadcasted_iota(jnp.int32, (each_row, positions), 1) + here * positions
    visible = jnp.concatenate([lane < lengths_ref[r] for r in range(rows)], axis=0)

    def all_lines(part):
        return jnp.concatenate([part(r, j) for r in range(rows) for j in range(KVH)], axis=0)

    def head_of(ref, r, j):
        return ref[r, :, j * HD : (j + 1) * HD]

    for copy in first:
        copy.wait()
    queries = []
    for r in range(rows):
        row = q[r].astype(jnp.float32)
        queries += [row[:, h * HD : (h + 1) * HD] for h in range(HQ)]
    queries = jnp.concatenate(queries, axis=0)
    narrow = queries.astype(jnp.bfloat16)

    def fresh_of(ref, t):
        return all_lines(
            lambda r, j: jnp.broadcast_to(ref[r, t : t + 1, j * HD : (j + 1) * HD].astype(jnp.float32), (block, HD))
        )

    fresh = [
        jnp.where(fresh_ok[t], jnp.sum(queries * fresh_of(nk, t), axis=1, keepdims=True) * HD**-0.5, masked_score)
        for t in range(2)
    ]
    for copy in keys:
        copy.wait()

    def lines_of(array, r, j):
        at = (r * KVH + j) * block
        return array[at : at + block]

    turned = (((1,), (1,)), ((), ()))
    scores = all_lines(
        lambda r, j: lax.dot_general(
            lines_of(narrow, r, j), head_of(k, r, j), turned, preferred_element_type=jnp.float32
        )
    )
    scores = jnp.where(visible, scores * HD**-0.5, masked_score)
    top = jnp.maximum(jnp.max(scores, axis=1, keepdims=True), jnp.maximum(*fresh))
    shift = top.astype(jnp.bfloat16).astype(jnp.float32)
    weights = jnp.where(visible, jnp.exp(scores - shift), 0.0)
    added = [jnp.where(fresh_ok[t], jnp.exp(fresh[t] - shift), 0.0) for t in range(2)]
    total = jnp.sum(weights, axis=1, keepdims=True) + added[0] + added[1]
    weights = weights.astype(jnp.bfloat16)
    for copy in values:
        copy.wait()
    accum = all_lines(
        lambda r, j: jnp.dot(lines_of(weights, r, j), head_of(v, r, j), preferred_element_type=jnp.float32)
    )
    for t in range(2):
        accum += added[t].astype(jnp.bfloat16).astype(jnp.float32) * fresh_of(nv, t)
    high = total.astype(jnp.bfloat16).astype(jnp.float32)
    line = lax.broadcasted_iota(jnp.int32, (LINES, HD), 0)
    offset = lax.broadcasted_iota(jnp.int32, (LINES, HD), 1) - line
    for half in range(2):
        for near in range(NEAR):

            def lines_to(array):
                parts = []
                for r in range(half * rows // 2, (half + 1) * rows // 2):
                    for side in range(2):
                        at = (r * KVH + side * 2 + near // 2) * block + near % 2 * 8
                        parts.append(array[at : at + 8])
                return jnp.concatenate(parts, axis=0)

            lead = lines_to(high)
            stats = jnp.where(offset == 0, lines_to(shift), 0.0)
            stats = jnp.where(offset == LINES, lead, stats)
            stats = jnp.where(offset == 2 * LINES, lines_to(total) - lead, stats)
            stats = jnp.broadcast_to(jnp.sum(stats, axis=0, keepdims=True), (8, HD))
            whole = jnp.concatenate([lines_to(accum), stats], axis=0).astype(jnp.bfloat16)
            for far in range(FAR):
                out_ref[(half * FAR + far) * NEAR + near] = whole


def attention(queries, cache_keys, cache_values, new_keys, new_values, lengths, here):
    kinds = (queries, cache_keys, cache_values, new_keys, new_values)
    smem = pl.BlockSpec(memory_space=pltpu.SMEM)
    return pl.pallas_call(
        attend,
        out_shape=jax.ShapeDtypeStruct((2 * FAR * NEAR, LINES + 8, HD), jnp.bfloat16),
        in_specs=[smem, smem] + [pl.BlockSpec(memory_space=pl.ANY)] * 5,
        out_specs=pl.BlockSpec(memory_space=pltpu.VMEM),
        scratch_shapes=[pltpu.VMEM(a.shape, a.dtype) for a in kinds]
        + [pltpu.SemaphoreType.DMA((3,)), pltpu.SemaphoreType.DMA((2, queries.shape[0]))],
        cost_estimate=pl.CostEstimate(flops=10**8, bytes_accessed=1 << 20, transcendentals=1 << 15),
        name="attend",
    )(lengths, here, *kinds)


def layer(
    queries,
    cache_keys,
    cache_values,
    new_keys,
    new_values,
    lengths,
    residual,
    norm_gain,
    w_gate,
    w_down,
):
    rows, steps, features = queries.shape
    groups, halves = lax.axis_size(GRP), lax.axis_size("xh")
    tokens = rows * steps
    share = tokens // halves
    total_tokens = groups * tokens
    near, far = NEAR, FAR

    def moved(weights):
        halves = pad_to(weights.T.astype(jnp.bfloat16), 0, 2 * HALF).reshape(2, HALF, HD)
        return [traded(halves, turn) for turn in range(2)]

    gate_weights, down_weights = moved(w_gate), moved(w_down)

    here = lax.axis_index(TP).reshape(1)
    sent = attention(queries, cache_keys, cache_values, new_keys, new_values, lengths, here)

    half, deep = lax.axis_index("xh"), lax.axis_index("z1")
    mine = residual.reshape(halves, share, 2, near, 4, HD)
    mine = lax.dynamic_index_in_dim(lax.dynamic_index_in_dim(mine, half, 0, False), deep, 2, False).astype(jnp.float32)
    gain = lax.dynamic_index_in_dim(norm_gain.reshape(2, near, 4, HD), deep, 1, False)
    own_gain = gain.reshape(2, 2, 2, HD)[lax.axis_index("xl"), :, lax.axis_index("c")]
    own_gain = jnp.where(lax.axis_index("ya") < NEAR // 2, own_gain, own_gain[::-1]).reshape(2 * HD)
    first = (lax.axis_index("z2") == 0).astype(jnp.float32)
    pieces = exchange(sent, TP)

    stats = pieces[:, LINES, : 3 * LINES].astype(jnp.float32).reshape(-1, 3, LINES)
    joint = jnp.max(stats[:, 0], axis=0)
    factor = jnp.exp(stats[:, 0] - joint)
    total = jnp.sum(factor * (stats[:, 1] + stats[:, 2]), axis=0)
    context = jnp.sum(factor[..., None] * pieces[:, :LINES].astype(jnp.float32), axis=0) / total[:, None]
    context = jnp.transpose(context.reshape(rows // halves, 2, 4, steps, HD), (0, 3, 1, 2, 4))

    summed = mine + context.reshape(share, 2, 4, HD)
    gained = (summed * gain).astype(jnp.bfloat16).reshape(share, 2, 2, 2, HD)
    gained = jnp.transpose(gained, (1, 3, 0, 2, 4))
    ordered = jnp.stack([gained, gained[:, :, :, ::-1]], axis=1)
    ordered = jnp.broadcast_to(ordered[:, :, None, :, None], (2, 2, near, 2, halves, share, 2, HD))
    ordered = ordered.reshape(groups * halves, share, 2 * HD)
    kept = summed * first
    ordered, kept, own_gain = lax.optimization_barrier((ordered, kept, own_gain))
    arrived = exchange(ordered, WIDE)
    arrived = arrived.reshape(total_tokens, 2 * HD)

    unscaled = arrived.astype(jnp.float32) / own_gain
    squares = jnp.stack(two_words(jnp.sum(unscaled * unscaled, axis=-1)), axis=-1)
    turned = (((1,), (1,)), ((), ()))
    gate = sum(
        lax.dot_general(arrived[:, at * HD : (at + 1) * HD], w, turned, preferred_element_type=jnp.float32)
        for at, w in enumerate(gate_weights)
    )
    sent = jnp.concatenate([gate.astype(jnp.bfloat16), squares], axis=-1)
    depth = lax.axis_size(DEEP)
    sums = exchange(sent.reshape(depth, total_tokens // depth, -1), DEEP)
    sums = sums.astype(jnp.float32).sum(axis=0)
    mean_square = (sums[:, HALF] + sums[:, HALF + 1]) / features
    gate = sums[:, :HALF] * lax.rsqrt(mean_square + 1e-05)[:, None]
    hidden = jax.nn.silu(gate).astype(jnp.bfloat16)
    hidden = copies(hidden, DEEP)
    hidden = hidden.reshape(total_tokens, HALF)
    terms = jnp.concatenate(
        [jnp.dot(hidden, w, preferred_element_type=jnp.float32).astype(jnp.bfloat16) for w in down_weights], axis=-1
    )
    partial = exchange(terms.reshape(groups * halves, share, 2 * HD), WIDE)
    partial = partial.reshape(2, 2, near, 2, halves, share, 2, HD).astype(jnp.float32).sum(axis=(2, 4))
    mlp = partial[:, 0] + partial[:, 1, :, :, ::-1]
    mlp = jnp.transpose(mlp, (2, 0, 3, 1, 4)).reshape(share, 2, 4, HD)
    mixed = mlp + kept
    mixed = copies(mixed.astype(jnp.bfloat16).reshape(share, 8 * HD), TP)
    mixed = mixed.reshape(halves, far, near, share, 2, 4, HD).astype(jnp.float32).sum(axis=1)
    mixed = jnp.transpose(mixed, (0, 2, 3, 1, 4, 5))
    return mixed.astype(jnp.bfloat16).reshape(rows, steps, features)


def solution(mesh):
    fine = Mesh(mesh.devices.reshape(2, 4, 2, 2, 2, 3, 4), ("xl", "ya", "yb", "c", "xh", "z2", "z1"))
    return jax.shard_map(
        layer,
        mesh=fine,
        in_specs=(
            P(GRP, None, None),
            P(GRP, TP, None),
            P(GRP, TP, None),
            P(GRP, None, None),
            P(GRP, None, None),
            P(GRP),
            P(GRP, None, None),
            P(),
            P(GRP, TP),
            P(GRP, TP),
        ),
        out_specs=P(GRP, None, None),
        check_vma=False,
    )
```

```python
import jax
import jax.numpy as jnp
from jax import lax
from jax.experimental import pallas as pl
from jax.experimental.pallas import tpu as pltpu
from jax.sharding import Mesh
from jax.sharding import PartitionSpec as P


HD = 128
KVH = 4
HQ = 32
EACH = HQ // KVH
NEAR = 4
FAR = 3
LINES = 32
GRP = ("xl", "ya", "yb", "c")
TP = ("xh", "z2", "z1")
WIDE = ("xl", "ya", "yb", "c", "xh")
DEEP = ("xl", "c", "z1")
PIECE = 152
HALF = 2 * PIECE
masked_score = -1e30


def exchange(parts, axis):
    return lax.all_to_all(parts, axis, split_axis=0, concat_axis=0, tiled=True)


def copies(part, axis):
    return exchange(jnp.broadcast_to(part, (lax.axis_size(axis), *part.shape)), axis)


def two_words(value):
    high = value.astype(jnp.bfloat16)
    return high, (value - high.astype(jnp.float32)).astype(jnp.bfloat16)


def pad_to(array, axis, size):
    widths = [(0, 0)] * array.ndim
    widths[axis] = (0, size - array.shape[axis])
    return jnp.pad(array, widths)


def traded(pieces, turn):
    over, under = turn // 2, turn % 2
    moves = []
    for row in range(NEAR):
        for pair in range(2):
            for deep in range(NEAR):
                target = (deep // 2 ^ under) * 2 + deep % 2
                moves.append(((row * 2 + pair) * NEAR + deep, (target * 2 + (pair ^ over)) * NEAR + row))
    at = (lax.axis_index("z1") // 2 ^ under) * 2 + (lax.axis_index("yb") ^ over)
    sent = lax.dynamic_index_in_dim(pieces, at, 1, False)
    return lax.ppermute(sent, ("ya", "yb", "z1"), moves)


def attend(lengths_ref, here_ref, q_hbm, k_hbm, v_hbm, nk_hbm, nv_hbm, out_ref, q, k, v, nk, nv, small, large):
    rows, positions = k.shape[0], k.shape[1]
    pairs = ((q_hbm, q), (nk_hbm, nk), (nv_hbm, nv))
    first = [pltpu.make_async_copy(s, d, small.at[i]) for i, (s, d) in enumerate(pairs)]
    keys = [pltpu.make_async_copy(k_hbm.at[r], k.at[r], large.at[0, r]) for r in range(rows)]
    values = [pltpu.make_async_copy(v_hbm.at[r], v.at[r], large.at[1, r]) for r in range(rows)]
    for copy in first + keys + values:
        copy.start()
    here = here_ref[0]
    block = 2 * EACH
    lines = rows * KVH * block
    each_row = KVH * block
    step = lax.rem(lax.broadcasted_iota(jnp.int32, (lines, 1), 0), 2)
    fresh_ok = [(here == 0) & (step >= t) for t in range(2)]
    lane = lax.broadcasted_iota(jnp.int32, (each_row, positions), 1) + here * positions
    visible = jnp.concatenate([lane < lengths_ref[r] for r in range(rows)], axis=0)

    def all_lines(part):
        return jnp.concatenate([part(r, j) for r in range(rows) for j in range(KVH)], axis=0)

    def head_of(ref, r, j):
        return ref[r, :, j * HD : (j + 1) * HD]

    for copy in first:
        copy.wait()
    queries = []
    for r in range(rows):
        row = q[r].astype(jnp.float32)
        queries += [row[:, h * HD : (h + 1) * HD] for h in range(HQ)]
    queries = jnp.concatenate(queries, axis=0)
    narrow = queries.astype(jnp.bfloat16)

    def fresh_of(ref, t):
        return all_lines(
            lambda r, j: jnp.broadcast_to(ref[r, t : t + 1, j * HD : (j + 1) * HD].astype(jnp.float32), (block, HD))
        )

    fresh = [
        jnp.where(fresh_ok[t], jnp.sum(queries * fresh_of(nk, t), axis=1, keepdims=True) * HD**-0.5, masked_score)
        for t in range(2)
    ]
    for copy in keys:
        copy.wait()

    def lines_of(array, r, j):
        at = (r * KVH + j) * block
        return array[at : at + block]

    turned = (((1,), (1,)), ((), ()))
    scores = all_lines(
        lambda r, j: lax.dot_general(
            lines_of(narrow, r, j), head_of(k, r, j), turned, preferred_element_type=jnp.float32
        )
    )
    scores = jnp.where(visible, scores * HD**-0.5, masked_score)
    top = jnp.maximum(jnp.max(scores, axis=1, keepdims=True), jnp.maximum(*fresh))
    shift = top.astype(jnp.bfloat16).astype(jnp.float32)
    weights = jnp.where(visible, jnp.exp(scores - shift), 0.0)
    added = [jnp.where(fresh_ok[t], jnp.exp(fresh[t] - shift), 0.0) for t in range(2)]
    total = jnp.sum(weights, axis=1, keepdims=True) + added[0] + added[1]
    weights = weights.astype(jnp.bfloat16)
    for copy in values:
        copy.wait()
    accum = all_lines(
        lambda r, j: jnp.dot(lines_of(weights, r, j), head_of(v, r, j), preferred_element_type=jnp.float32)
    )
    for t in range(2):
        accum += added[t].astype(jnp.bfloat16).astype(jnp.float32) * fresh_of(nv, t)
    high = total.astype(jnp.bfloat16).astype(jnp.float32)
    line = lax.broadcasted_iota(jnp.int32, (LINES, HD), 0)
    offset = lax.broadcasted_iota(jnp.int32, (LINES, HD), 1) - line
    for half in range(2):
        for near in range(NEAR):

            def lines_to(array):
                parts = []
                for r in range(half * rows // 2, (half + 1) * rows // 2):
                    for side in range(2):
                        at = (r * KVH + side * 2 + near // 2) * block + near % 2 * 8
                        parts.append(array[at : at + 8])
                return jnp.concatenate(parts, axis=0)

            lead = lines_to(high)
            stats = jnp.where(offset == 0, lines_to(shift), 0.0)
            stats = jnp.where(offset == LINES, lead, stats)
            stats = jnp.where(offset == 2 * LINES, lines_to(total) - lead, stats)
            stats = jnp.broadcast_to(jnp.sum(stats, axis=0, keepdims=True), (8, HD))
            whole = jnp.concatenate([lines_to(accum), stats], axis=0).astype(jnp.bfloat16)
            for far in range(FAR):
                out_ref[(half * FAR + far) * NEAR + near] = whole


def attention(queries, cache_keys, cache_values, new_keys, new_values, lengths, here):
    kinds = (queries, cache_keys, cache_values, new_keys, new_values)
    smem = pl.BlockSpec(memory_space=pltpu.SMEM)
    return pl.pallas_call(
        attend,
        out_shape=jax.ShapeDtypeStruct((2 * FAR * NEAR, LINES + 8, HD), jnp.bfloat16),
        in_specs=[smem, smem] + [pl.BlockSpec(memory_space=pl.ANY)] * 5,
        out_specs=pl.BlockSpec(memory_space=pltpu.VMEM),
        scratch_shapes=[pltpu.VMEM(a.shape, a.dtype) for a in kinds]
        + [pltpu.SemaphoreType.DMA((3,)), pltpu.SemaphoreType.DMA((2, queries.shape[0]))],
        cost_estimate=pl.CostEstimate(flops=10**8, bytes_accessed=1 << 20, transcendentals=1 << 15),
        name="attend",
    )(lengths, here, *kinds)


def layer(
    queries,
    cache_keys,
    cache_values,
    new_keys,
    new_values,
    lengths,
    residual,
    norm_gain,
    w_gate,
    w_down,
):
    rows, steps, features = queries.shape
    groups, halves = lax.axis_size(GRP), lax.axis_size("xh")
    tokens = rows * steps
    share = tokens // halves
    total_tokens = groups * tokens
    near, far = NEAR, FAR

    stacked = jnp.stack([w_gate.T, w_down.T]).astype(jnp.bfloat16)
    stacked = pad_to(stacked, 1, 4 * PIECE).reshape(2, 4, PIECE, HD)
    moved = [traded(stacked, turn) for turn in range(4)]

    here = lax.axis_index(TP).reshape(1)
    sent = attention(queries, cache_keys, cache_values, new_keys, new_values, lengths, here)

    half, deep = lax.axis_index("xh"), lax.axis_index("z1")
    mine = residual.reshape(halves, share, 2, near, 4, HD)
    mine = lax.dynamic_index_in_dim(lax.dynamic_index_in_dim(mine, half, 0, False), deep, 2, False).astype(jnp.float32)
    gain = lax.dynamic_index_in_dim(norm_gain.reshape(2, near, 4, HD), deep, 1, False)
    own_gain = gain.reshape(2, 2, 2, HD)[lax.axis_index("xl"), :, lax.axis_index("c")]
    own_gain = jnp.where(lax.axis_index("yb") == 0, own_gain, own_gain[::-1]).reshape(2 * HD)
    first = (lax.axis_index("z2") == 0).astype(jnp.float32)
    pieces = exchange(sent, TP)

    stats = pieces[:, LINES, : 3 * LINES].astype(jnp.float32).reshape(-1, 3, LINES)
    joint = jnp.max(stats[:, 0], axis=0)
    factor = jnp.exp(stats[:, 0] - joint)
    total = jnp.sum(factor * (stats[:, 1] + stats[:, 2]), axis=0)
    context = jnp.sum(factor[..., None] * pieces[:, :LINES].astype(jnp.float32), axis=0) / total[:, None]
    context = jnp.transpose(context.reshape(rows // halves, 2, 4, steps, HD), (0, 3, 1, 2, 4))

    summed = mine + context.reshape(share, 2, 4, HD)
    gained = (summed * gain).astype(jnp.bfloat16).reshape(share, 2, 2, 2, HD)
    gained = jnp.transpose(gained, (1, 3, 0, 2, 4))
    ordered = jnp.stack([gained, gained[:, :, :, ::-1]], axis=1)
    ordered = jnp.broadcast_to(ordered[:, None, :, :, None], (2, near, 2, 2, halves, share, 2, HD))
    ordered = ordered.reshape(groups * halves, share, 2 * HD)
    kept = summed * first
    ordered, kept, own_gain = lax.optimization_barrier((ordered, kept, own_gain))
    arrived = exchange(ordered, WIDE)
    arrived = arrived.reshape(total_tokens, 2 * HD)

    unscaled = arrived.astype(jnp.float32) / own_gain
    squares = jnp.stack(two_words(jnp.sum(unscaled * unscaled, axis=-1)), axis=-1)
    squares, moved = lax.optimization_barrier((squares, moved))
    turned = (((1,), (1,)), ((), ()))
    gate_weights, down_weights = (
        [jnp.concatenate([moved[2 * block][kind], moved[2 * block + 1][kind]], axis=0) for block in range(2)]
        for kind in range(2)
    )
    gate = sum(
        lax.dot_general(arrived[:, at * HD : (at + 1) * HD], w, turned, preferred_element_type=jnp.float32)
        for at, w in enumerate(gate_weights)
    )
    sent = jnp.concatenate([gate.astype(jnp.bfloat16), squares], axis=-1)
    depth = lax.axis_size(DEEP)
    sums = exchange(sent.reshape(depth, total_tokens // depth, -1), DEEP).astype(jnp.float32).sum(axis=0)
    mean_square = (sums[:, HALF] + sums[:, HALF + 1]) / features
    gate = sums[:, :HALF] * lax.rsqrt(mean_square + 1e-05)[:, None]
    hidden = copies(jax.nn.silu(gate).astype(jnp.bfloat16), DEEP).reshape(total_tokens, HALF)
    terms = jnp.concatenate(
        [jnp.dot(hidden, w, preferred_element_type=jnp.float32).astype(jnp.bfloat16) for w in down_weights], axis=-1
    )
    partial = exchange(terms.reshape(groups * halves, share, 2 * HD), WIDE)
    partial = partial.reshape(2, near, 2, 2, halves, share, 2, HD).astype(jnp.float32).sum(axis=(1, 4))
    mlp = partial[:, 0] + partial[:, 1, :, :, ::-1]
    mlp = jnp.transpose(mlp, (2, 0, 3, 1, 4)).reshape(share, 2, 4, HD)
    mixed = mlp + kept
    mixed = copies(mixed.astype(jnp.bfloat16).reshape(share, 8 * HD), TP)
    mixed = mixed.reshape(halves, far, near, share, 2, 4, HD).astype(jnp.float32).sum(axis=1)
    mixed = jnp.transpose(mixed, (0, 2, 3, 1, 4, 5))
    return mixed.astype(jnp.bfloat16).reshape(rows, steps, features)


def solution(mesh):
    fine = Mesh(mesh.devices.reshape(2, 4, 2, 2, 2, 3, 4), ("xl", "ya", "yb", "c", "xh", "z2", "z1"))
    return jax.shard_map(
        layer,
        mesh=fine,
        in_specs=(
            P(GRP, None, None),
            P(GRP, TP, None),
            P(GRP, TP, None),
            P(GRP, None, None),
            P(GRP, None, None),
            P(GRP),
            P(GRP, None, None),
            P(),
            P(GRP, TP),
            P(GRP, TP),
        ),
        out_specs=P(GRP, None, None),
        check_vma=False,
    )
```

```python
import jax
import jax.numpy as jnp
from jax import lax
from jax.experimental import pallas as pl
from jax.experimental.pallas import tpu as pltpu
from jax.sharding import Mesh
from jax.sharding import PartitionSpec as P


HD = 128
KVH = 4
HQ = 32
EACH = HQ // KVH
NEAR = 4
FAR = 3
LINES = 32
GRP = ("xl", "yb", "ya", "c")
TP = ("xh", "z2", "z1")
WIDE = ("xl", "yb", "ya", "c", "xh")
DEEP = ("xl", "c", "z1")
HALF = 304
masked_score = -1e30


def exchange(parts, axis):
    return lax.all_to_all(parts, axis, split_axis=0, concat_axis=0, tiled=True)


def copies(part, axis):
    return exchange(jnp.broadcast_to(part, (lax.axis_size(axis), *part.shape)), axis)


def two_words(value):
    high = value.astype(jnp.bfloat16)
    return high, (value - high.astype(jnp.float32)).astype(jnp.bfloat16)


def pad_to(array, axis, size):
    widths = [(0, 0)] * array.ndim
    widths[axis] = (0, size - array.shape[axis])
    return jnp.pad(array, widths)


def traded(halves, turn):
    moves = []
    for row in range(NEAR):
        for pair in range(2):
            for deep in range(NEAR):
                target = (pair ^ turn) * NEAR + deep
                moves.append(((pair * NEAR + row) * NEAR + deep, target * NEAR + row))
    sent = lax.dynamic_index_in_dim(halves, lax.axis_index("yb") ^ turn, 1, False)
    return lax.ppermute(sent, ("yb", "ya", "z1"), moves)


def attend(lengths_ref, here_ref, q_hbm, k_hbm, v_hbm, nk_hbm, nv_hbm, out_ref, q, k, v, nk, nv, small, large):
    rows, positions = k.shape[0], k.shape[1]
    pairs = ((q_hbm, q), (nk_hbm, nk), (nv_hbm, nv))
    first = [pltpu.make_async_copy(s, d, small.at[i]) for i, (s, d) in enumerate(pairs)]
    keys = [pltpu.make_async_copy(k_hbm.at[r], k.at[r], large.at[0, r]) for r in range(rows)]
    values = [pltpu.make_async_copy(v_hbm.at[r], v.at[r], large.at[1, r]) for r in range(rows)]
    for copy in first + keys + values:
        copy.start()
    here = here_ref[0]
    block = 2 * EACH
    lines = rows * KVH * block
    each_row = KVH * block
    step = lax.rem(lax.broadcasted_iota(jnp.int32, (lines, 1), 0), 2)
    fresh_ok = [(here == 0) & (step >= t) for t in range(2)]
    lane = lax.broadcasted_iota(jnp.int32, (each_row, positions), 1) + here * positions
    visible = jnp.concatenate([lane < lengths_ref[r] for r in range(rows)], axis=0)

    def all_lines(part):
        return jnp.concatenate([part(r, j) for r in range(rows) for j in range(KVH)], axis=0)

    def head_of(ref, r, j):
        return ref[r, :, j * HD : (j + 1) * HD]

    for copy in first:
        copy.wait()
    queries = []
    for r in range(rows):
        row = q[r].astype(jnp.float32)
        queries += [row[:, h * HD : (h + 1) * HD] for h in range(HQ)]
    queries = jnp.concatenate(queries, axis=0)
    narrow = queries.astype(jnp.bfloat16)

    def fresh_of(ref, t):
        return all_lines(
            lambda r, j: jnp.broadcast_to(ref[r, t : t + 1, j * HD : (j + 1) * HD].astype(jnp.float32), (block, HD))
        )

    fresh = [
        jnp.where(fresh_ok[t], jnp.sum(queries * fresh_of(nk, t), axis=1, keepdims=True) * HD**-0.5, masked_score)
        for t in range(2)
    ]
    for copy in keys:
        copy.wait()

    def lines_of(array, r, j):
        at = (r * KVH + j) * block
        return array[at : at + block]

    turned = (((1,), (1,)), ((), ()))
    scores = all_lines(
        lambda r, j: lax.dot_general(
            lines_of(narrow, r, j), head_of(k, r, j), turned, preferred_element_type=jnp.float32
        )
    )
    scores = jnp.where(visible, scores * HD**-0.5, masked_score)
    top = jnp.maximum(jnp.max(scores, axis=1, keepdims=True), jnp.maximum(*fresh))
    shift = top.astype(jnp.bfloat16).astype(jnp.float32)
    weights = jnp.where(visible, jnp.exp(scores - shift), 0.0)
    added = [jnp.where(fresh_ok[t], jnp.exp(fresh[t] - shift), 0.0) for t in range(2)]
    total = jnp.sum(weights, axis=1, keepdims=True) + added[0] + added[1]
    weights = weights.astype(jnp.bfloat16)
    for copy in values:
        copy.wait()
    accum = all_lines(
        lambda r, j: jnp.dot(lines_of(weights, r, j), head_of(v, r, j), preferred_element_type=jnp.float32)
    )
    for t in range(2):
        accum += added[t].astype(jnp.bfloat16).astype(jnp.float32) * fresh_of(nv, t)
    high = total.astype(jnp.bfloat16).astype(jnp.float32)
    line = lax.broadcasted_iota(jnp.int32, (LINES, HD), 0)
    offset = lax.broadcasted_iota(jnp.int32, (LINES, HD), 1) - line
    for half in range(2):
        for near in range(NEAR):

            def lines_to(array):
                parts = []
                for r in range(half * rows // 2, (half + 1) * rows // 2):
                    for j in range(KVH):
                        at = (r * KVH + j) * block + near * 4
                        parts.append(array[at : at + 4])
                return jnp.concatenate(parts, axis=0)

            lead = lines_to(high)
            stats = jnp.where(offset == 0, lines_to(shift), 0.0)
            stats = jnp.where(offset == LINES, lead, stats)
            stats = jnp.where(offset == 2 * LINES, lines_to(total) - lead, stats)
            stats = jnp.broadcast_to(jnp.sum(stats, axis=0, keepdims=True), (8, HD))
            whole = jnp.concatenate([lines_to(accum), stats], axis=0).astype(jnp.bfloat16)
            for far in range(FAR):
                out_ref[(half * FAR + far) * NEAR + near] = whole


def attention(queries, cache_keys, cache_values, new_keys, new_values, lengths, here):
    kinds = (queries, cache_keys, cache_values, new_keys, new_values)
    smem = pl.BlockSpec(memory_space=pltpu.SMEM)
    return pl.pallas_call(
        attend,
        out_shape=jax.ShapeDtypeStruct((2 * FAR * NEAR, LINES + 8, HD), jnp.bfloat16),
        in_specs=[smem, smem] + [pl.BlockSpec(memory_space=pl.ANY)] * 5,
        out_specs=pl.BlockSpec(memory_space=pltpu.VMEM),
        scratch_shapes=[pltpu.VMEM(a.shape, a.dtype) for a in kinds]
        + [pltpu.SemaphoreType.DMA((3,)), pltpu.SemaphoreType.DMA((2, queries.shape[0]))],
        cost_estimate=pl.CostEstimate(flops=10**8, bytes_accessed=1 << 20, transcendentals=1 << 15),
        name="attend",
    )(lengths, here, *kinds)


def layer(
    queries,
    cache_keys,
    cache_values,
    new_keys,
    new_values,
    lengths,
    residual,
    norm_gain,
    w_gate,
    w_down,
):
    rows, steps, features = queries.shape
    groups, halves = lax.axis_size(GRP), lax.axis_size("xh")
    tokens = rows * steps
    share = tokens // halves
    total_tokens = groups * tokens
    near, far = NEAR, FAR

    stacked = jnp.stack([w_gate.T, w_down.T]).astype(jnp.bfloat16)
    halves_of = pad_to(stacked, 1, 2 * HALF).reshape(2, 2, HALF, HD)
    moved = [traded(halves_of, turn) for turn in range(2)]
    gate_weights, down_weights = ([pieces[kind] for pieces in moved] for kind in range(2))

    here = lax.axis_index(TP).reshape(1)
    sent = attention(queries, cache_keys, cache_values, new_keys, new_values, lengths, here)

    half, deep = lax.axis_index("xh"), lax.axis_index("z1")
    mine = residual.reshape(halves, share, 2, 2, near, 2, HD)
    mine = lax.dynamic_index_in_dim(lax.dynamic_index_in_dim(mine, half, 0, False), deep, 3, False).astype(jnp.float32)
    mine = mine.reshape(share, 2, 4, HD)
    gain = lax.dynamic_index_in_dim(norm_gain.reshape(2, 2, near, 2, HD), deep, 2, False).reshape(2, 4, HD)
    own_gain = gain.reshape(2, 2, 2, HD)[lax.axis_index("xl"), :, lax.axis_index("c")]
    own_gain = jnp.where(lax.axis_index("yb") == 0, own_gain, own_gain[::-1]).reshape(2 * HD)
    first = (lax.axis_index("z2") == 0).astype(jnp.float32)
    pieces = exchange(sent, TP)

    stats = pieces[:, LINES, : 3 * LINES].astype(jnp.float32).reshape(-1, 3, LINES)
    joint = jnp.max(stats[:, 0], axis=0)
    factor = jnp.exp(stats[:, 0] - joint)
    total = jnp.sum(factor * (stats[:, 1] + stats[:, 2]), axis=0)
    context = jnp.sum(factor[..., None] * pieces[:, :LINES].astype(jnp.float32), axis=0) / total[:, None]
    context = jnp.transpose(context.reshape(rows // halves, 2, 4, steps, HD), (0, 3, 1, 2, 4))

    summed = mine + context.reshape(share, 2, 4, HD)
    gained = (summed * gain).astype(jnp.bfloat16).reshape(share, 2, 2, 2, HD)
    gained = jnp.transpose(gained, (1, 3, 0, 2, 4))
    ordered = jnp.stack([gained, gained[:, :, :, ::-1]], axis=1)
    ordered = jnp.broadcast_to(ordered[:, :, None, :, None], (2, 2, near, 2, halves, share, 2, HD))
    ordered = ordered.reshape(groups * halves, share, 2 * HD)
    kept = summed * first
    ordered, kept, own_gain = lax.optimization_barrier((ordered, kept, own_gain))
    arrived = exchange(ordered, WIDE)
    arrived = arrived.reshape(total_tokens, 2 * HD)

    unscaled = arrived.astype(jnp.float32) / own_gain
    squares = jnp.stack(two_words(jnp.sum(unscaled * unscaled, axis=-1)), axis=-1)
    turned = (((1,), (1,)), ((), ()))
    gate = sum(
        lax.dot_general(arrived[:, at * HD : (at + 1) * HD], w, turned, preferred_element_type=jnp.float32)
        for at, w in enumerate(gate_weights)
    )
    sent = jnp.concatenate([gate.astype(jnp.bfloat16), squares], axis=-1)
    depth = lax.axis_size(DEEP)
    sums = exchange(sent.reshape(depth, total_tokens // depth, -1), DEEP).astype(jnp.float32).sum(axis=0)
    mean_square = (sums[:, HALF] + sums[:, HALF + 1]) / features
    gate = sums[:, :HALF] * lax.rsqrt(mean_square + 1e-05)[:, None]
    hidden = jax.nn.silu(gate).astype(jnp.bfloat16)
    hidden = copies(hidden, DEEP).reshape(total_tokens, HALF)
    terms = jnp.concatenate(
        [jnp.dot(hidden, w, preferred_element_type=jnp.float32).astype(jnp.bfloat16) for w in down_weights], axis=-1
    )
    partial = exchange(terms.reshape(groups * halves, share, 2 * HD), WIDE)
    partial = partial.reshape(2, 2, near, 2, halves, share, 2, HD).astype(jnp.float32).sum(axis=(2, 4))
    mlp = partial[:, 0] + partial[:, 1, :, :, ::-1]
    mlp = jnp.transpose(mlp, (2, 0, 3, 1, 4)).reshape(share, 2, 4, HD)
    mixed = mlp + kept
    mixed = copies(mixed.astype(jnp.bfloat16).reshape(share, 8 * HD), TP)
    mixed = mixed.reshape(halves, far, near, share, 2, 2, 2, HD).astype(jnp.float32).sum(axis=1)
    mixed = jnp.transpose(mixed, (0, 2, 3, 4, 1, 5, 6))
    return mixed.astype(jnp.bfloat16).reshape(rows, steps, features)


def solution(mesh):
    fine = Mesh(mesh.devices.reshape(2, 2, 4, 2, 2, 3, 4), ("xl", "yb", "ya", "c", "xh", "z2", "z1"))
    return jax.shard_map(
        layer,
        mesh=fine,
        in_specs=(
            P(GRP, None, None),
            P(GRP, TP, None),
            P(GRP, TP, None),
            P(GRP, None, None),
            P(GRP, None, None),
            P(GRP),
            P(GRP, None, None),
            P(),
            P(GRP, TP),
            P(GRP, TP),
        ),
        out_specs=P(GRP, None, None),
        check_vma=False,
    )
```
